8 devices in a mesh: stage: 2 (over z, y), expert: 4 (over x, core).
Axes of the slice: x: 2, y: 2, z: 1, core: 2. Of those that a mesh axis runs over, the one named last changes fastest.
Arguments:
- x_act: bfloat16 [2, 8192, 512], P('stage', 'expert')
- route_idx: int32 [2, 8192, 8], P('stage', 'expert')
- route_wts: float32 [2, 8192, 8], P('stage', 'expert')
- w_one: bfloat16 [2, 128, 512, 768], P('stage', 'expert')
- w_three: bfloat16 [2, 128, 512, 768], P('stage', 'expert')
- w_two: bfloat16 [2, 128, 768, 512], P('stage', 'expert')
- dy_act: bfloat16 [2, 8192, 512], P('stage', 'expert')
Outputs:
- output 1: bfloat16 [2, 8192, 512], P('stage', 'expert')
- output 2: bfloat16 [2, 8192, 512], P('stage', 'expert')
- output 3: bfloat16 [2, 128, 512, 768], P('stage', 'expert')
- output 4: bfloat16 [2, 128, 512, 768], P('stage', 'expert')
- output 5: bfloat16 [2, 128, 768, 512], P('stage', 'expert')
All inputs are finite; a program needn't handle non-finite values.
Results may differ from the reference program's by a relative error of at most 0.0149914.
Values are sent between devices in bfloat16 or wider.
A program may use at most 1 GiB of HBM per device.

```python
import jax
import jax.numpy as jnp
from jax import lax

STAGES = 2
EXPERT_DEVS = 4
TOK_DEV = 2048
MODEL_DIM = 512
FFN_DIM = 768
EXPERTS = 128
TOP_K = 8
ROUTE_DEVS = 8

LOCAL_EXP = EXPERTS // EXPERT_DEVS
CAPACITY = 2 * TOK_DEV * TOP_K // EXPERTS - 1
TOKENS = EXPERT_DEVS * TOK_DEV
N_SLOT = TOK_DEV * TOP_K


def draw_routing(rng_key):
    n_blocks = EXPERTS // TOP_K
    mean_load = TOK_DEV * TOP_K // EXPERTS
    group_devs = min(ROUTE_DEVS, EXPERT_DEVS)
    group_exp = group_devs * LOCAL_EXP
    key_pair, key_shift, key_tok, key_grp, key_dev = jax.random.split(rng_key, 5)
    block_ids = jnp.broadcast_to(jnp.arange(n_blocks, dtype=jnp.int32), (STAGES, n_blocks))
    pair_perm = jax.random.permutation(key_pair, block_ids, axis=1, independent=True)
    shifts = jax.random.randint(key_shift, (STAGES, EXPERT_DEVS, n_blocks // 2), 0, mean_load)
    shifts = shifts.at[:, :, 0].set(mean_load - 1)
    pair_sign = jnp.array([1, -1], dtype=jnp.int32)
    delta_pos = (shifts[:, :, :, None] * pair_sign).reshape(STAGES, EXPERT_DEVS, n_blocks)
    inv_perm = jnp.broadcast_to(jnp.argsort(pair_perm, axis=1)[:, None, :], delta_pos.shape)
    blk_load = mean_load + jnp.take_along_axis(delta_pos, inv_perm, axis=2)
    blk_ends = jnp.cumsum(blk_load, axis=2)
    tok_pos = jnp.arange(TOK_DEV, dtype=jnp.int32)
    blk_of = jnp.sum((blk_ends[:, :, None, :] <= tok_pos[None, None, :, None]).astype(jnp.int32), axis=3)
    blk_of = jax.random.permutation(key_tok, blk_of, axis=2, independent=True)
    virt_ids = blk_of[:, :, :, None] * TOP_K + jnp.arange(TOP_K, dtype=jnp.int32)
    virt_flat = virt_ids.reshape(STAGES, TOKENS * TOP_K)
    inner_ids = jnp.broadcast_to(jnp.arange(group_exp, dtype=jnp.int32), (STAGES, EXPERTS // group_exp, group_exp))
    grp_perm = jax.random.permutation(key_grp, inner_ids, axis=2, independent=True).reshape(STAGES, EXPERTS)
    dev_ids = jnp.broadcast_to(jnp.arange(EXPERT_DEVS, dtype=jnp.int32), (STAGES, EXPERT_DEVS))
    dev_perm = jax.random.permutation(key_dev, dev_ids, axis=1, independent=True)
    in_group = jnp.take_along_axis(grp_perm, virt_flat, axis=1)
    pre_dev = (virt_flat // group_exp) * group_devs + in_group // LOCAL_EXP
    dest_dev = jnp.take_along_axis(dev_perm, pre_dev, axis=1)
    expert_id = dest_dev * LOCAL_EXP + in_group % LOCAL_EXP
    return expert_id.reshape(STAGES, TOKENS, TOP_K)


def setup_inputs(seed: int = 0) -> dict:
    rng_key = jax.random.key(seed)
    key_x, key_idx, key_wts, key_one, key_three, key_two, key_dy = jax.random.split(rng_key, 7)
    x_act = jax.random.normal(key_x, (STAGES, TOKENS, MODEL_DIM), jnp.float32)
    route_idx = draw_routing(key_idx)
    route_wts = jax.random.uniform(key_wts, (STAGES, TOKENS, TOP_K), jnp.float32, 0.5, 1.5)
    w_one = jax.random.normal(key_one, (STAGES, EXPERTS, MODEL_DIM, FFN_DIM), jnp.float32) * MODEL_DIM ** -0.5
    w_three = jax.random.normal(key_three, (STAGES, EXPERTS, MODEL_DIM, FFN_DIM), jnp.float32) * MODEL_DIM ** -0.5
    w_two = jax.random.normal(key_two, (STAGES, EXPERTS, FFN_DIM, MODEL_DIM), jnp.float32) * FFN_DIM ** -0.5
    dy_act = jax.random.normal(key_dy, (STAGES, TOKENS, MODEL_DIM), jnp.float32)
    return {
        'x_act': x_act.astype(jnp.bfloat16),
        'route_idx': route_idx,
        'route_wts': route_wts,
        'w_one': w_one.astype(jnp.bfloat16),
        'w_three': w_three.astype(jnp.bfloat16),
        'w_two': w_two.astype(jnp.bfloat16),
        'dy_act': dy_act.astype(jnp.bfloat16),
    }


def take_rows(row_table, row_ids):
    return jnp.take(row_table, row_ids, axis=0, mode='fill', fill_value=0)


def stage_tables(idx_blk):
    slot_ids = idx_blk.reshape(N_SLOT)
    hit_mat = (slot_ids[:, None] == jnp.arange(EXPERTS, dtype=jnp.int32)[None, :]).astype(jnp.int32)
    slot_rank = jnp.sum(jnp.cumsum(hit_mat, axis=0) * hit_mat, axis=1) - 1
    buf_pos = slot_ids * CAPACITY + slot_rank
    slot_at = jnp.full((EXPERTS * CAPACITY,), N_SLOT, jnp.int32).at[buf_pos].set(jnp.arange(N_SLOT, dtype=jnp.int32))
    return buf_pos, slot_at


def one_expert(operands):
    x_rows, d_rows, w_in_one, w_in_three, w_out = operands
    pre_one = jnp.dot(x_rows, w_in_one, preferred_element_type=jnp.float32)
    pre_three = jnp.dot(x_rows, w_in_three, preferred_element_type=jnp.float32)
    sig_one = jax.nn.sigmoid(pre_one)
    act_one = pre_one * sig_one
    hidden = (act_one * pre_three).astype(jnp.bfloat16)
    out_rows = jnp.dot(hidden, w_out, preferred_element_type=jnp.float32).astype(jnp.bfloat16)
    d_hidden = jnp.dot(d_rows, w_out.T, preferred_element_type=jnp.float32).astype(jnp.bfloat16).astype(jnp.float32)
    d_three = (d_hidden * act_one).astype(jnp.bfloat16)
    d_one = (d_hidden * pre_three * sig_one * (1.0 + pre_one * (1.0 - sig_one))).astype(jnp.bfloat16)
    dx_rows = (jnp.dot(d_one, w_in_one.T, preferred_element_type=jnp.float32) + jnp.dot(d_three, w_in_three.T, preferred_element_type=jnp.float32)).astype(jnp.bfloat16)
    g_one = jnp.dot(x_rows.T, d_one, preferred_element_type=jnp.float32).astype(jnp.bfloat16)
    g_three = jnp.dot(x_rows.T, d_three, preferred_element_type=jnp.float32).astype(jnp.bfloat16)
    g_two = jnp.dot(hidden.T, d_rows, preferred_element_type=jnp.float32).astype(jnp.bfloat16)
    return out_rows, dx_rows, g_one, g_three, g_two


def to_experts(rows):
    return jnp.transpose(rows.reshape(EXPERT_DEVS, EXPERTS, CAPACITY, MODEL_DIM), (1, 0, 2, 3)).reshape(EXPERTS, EXPERT_DEVS * CAPACITY, MODEL_DIM)


def from_experts(rows):
    return jnp.transpose(rows.reshape(EXPERTS, EXPERT_DEVS, CAPACITY, MODEL_DIM), (1, 0, 2, 3)).reshape(EXPERT_DEVS, EXPERTS * CAPACITY, MODEL_DIM)


def stage_layer(operands):
    x_in, idx_in, wts_in, w_one, w_three, w_two, dy_in = operands
    buf_pos, slot_at = lax.map(stage_tables, idx_in.reshape(EXPERT_DEVS, TOK_DEV, TOP_K))
    x_dev = x_in.reshape(EXPERT_DEVS, TOK_DEV, MODEL_DIM)
    wts_dev = wts_in.reshape(EXPERT_DEVS, TOK_DEV, TOP_K)
    dy_dev = dy_in.reshape(EXPERT_DEVS, TOK_DEV, 1, MODEL_DIM)
    d_slot = (wts_dev[:, :, :, None] * dy_dev.astype(jnp.float32)).astype(jnp.bfloat16).reshape(EXPERT_DEVS, N_SLOT, MODEL_DIM)
    x_exp = to_experts(jax.vmap(take_rows)(x_dev, slot_at // TOP_K))
    d_exp = to_experts(jax.vmap(take_rows)(d_slot, slot_at))
    out_exp, dx_exp, dw_one, dw_three, dw_two = lax.map(one_expert, (x_exp, d_exp, w_one, w_three, w_two))
    out_slot = jax.vmap(take_rows)(from_experts(out_exp), buf_pos).reshape(EXPERT_DEVS, TOK_DEV, TOP_K, MODEL_DIM)
    dx_slot = jax.vmap(take_rows)(from_experts(dx_exp), buf_pos).reshape(EXPERT_DEVS, TOK_DEV, TOP_K, MODEL_DIM)
    y_out = jnp.sum(wts_dev[:, :, :, None] * out_slot.astype(jnp.float32), axis=2).astype(jnp.bfloat16)
    dx_out = jnp.sum(dx_slot.astype(jnp.float32), axis=2).astype(jnp.bfloat16)
    return y_out.reshape(TOKENS, MODEL_DIM), dx_out.reshape(TOKENS, MODEL_DIM), dw_one, dw_three, dw_two


def reference(x_act, route_idx, route_wts, w_one, w_three, w_two, dy_act):
    x_in = jnp.roll(x_act, 1, axis=0)
    idx_in = jnp.roll(route_idx, 1, axis=0)
    wts_in = jnp.roll(route_wts, 1, axis=0)
    y_act, dx_dst, dw_one, dw_three, dw_two = lax.map(stage_layer, (x_in, idx_in, wts_in, w_one, w_three, w_two, dy_act))
    dx_act = jnp.roll(dx_dst, -1, axis=0)
    return (y_act, dx_act, dw_one, dw_three, dw_two)
```

```python
import functools

import jax
import jax.numpy as jnp
from jax import lax
from jax.experimental import pallas as pl
from jax.experimental.pallas import tpu as pltpu
from jax.sharding import PartitionSpec as P


F32 = jnp.float32
BF16 = jnp.bfloat16
LIST = 264
PER_SRC = 256
TILE = 256
LANES = 128
STAGE_ROWS = 512
VMEM_LIMIT = 66 * 1000 * 1000


def dot_nn(a, b):
    return lax.dot_general(a, b, (((1,), (0,)), ((), ())), preferred_element_type=F32)


def dot_nt(a, b):
    return lax.dot_general(a, b, (((1,), (1,)), ((), ())), preferred_element_type=F32)


def dot_tn(a, b):
    return lax.dot_general(a, b, (((0,), (0,)), ((), ())), preferred_element_type=F32)


def route_kernel(n_tok, top_k, n_exp, dummy, base_ref, idx_ref, wts_ref, tok_ref, g_ref, cnt_ref):
    base = base_ref[0]

    @pl.loop(0, n_exp)
    def _(e):
        cnt_ref[e] = 0

    @pl.loop(0, n_tok)
    def _(t):
        experts = [idx_ref[t * top_k + j] for j in range(top_k)]
        ranks = [cnt_ref[e] for e in experts]
        wts = [wts_ref[t * top_k + j] for j in range(top_k)]
        for e, r, w in zip(experts, ranks, wts):
            tok_ref[e * LIST + r] = base + t
            g_ref[e * LIST + r] = w
            cnt_ref[e] = r + 1

    @pl.loop(0, n_exp)
    def _(e):
        r = cnt_ref[e]
        for k in range(7):
            tok_ref[e * LIST + r + k] = dummy
            g_ref[e * LIST + r + k] = 0.0
        tok_ref[e * LIST + LIST - 1] = r


def route_lists(idx, wts, base, n_exp, dummy):
    n_tok, top_k = idx.shape
    smem = pl.BlockSpec(memory_space=pltpu.SMEM)
    return pl.pallas_call(
        functools.partial(route_kernel, n_tok, top_k, n_exp, dummy),
        out_shape=(jax.ShapeDtypeStruct((n_exp * LIST,), jnp.int32), jax.ShapeDtypeStruct((n_exp * LIST,), F32)),
        in_specs=[smem, smem, smem],
        out_specs=(smem, smem),
        scratch_shapes=[pltpu.SMEM((n_exp,), jnp.int32)],
        cost_estimate=pl.CostEstimate(flops=60 * 10**8, bytes_accessed=4 * n_exp * LIST * 4, transcendentals=0),
        name='route_lists',
    )(base.reshape(1), idx.reshape(n_tok * top_k), wts.reshape(n_tok * top_k))


def load_table(src_hbm, table, stage, sem, n_rows, n_col):
    n_chunk = n_rows // STAGE_ROWS

    def fetch(i):
        slot = lax.rem(i, 2)
        return pltpu.make_async_copy(src_hbm.at[pl.ds(pl.multiple_of(i * STAGE_ROWS, STAGE_ROWS), STAGE_ROWS)], stage.at[slot], sem.at[slot])

    fetch(0).start()

    @pl.loop(0, n_chunk)
    def _(i):
        @pl.when(i + 1 < n_chunk)
        def _():
            fetch(i + 1).start()

        fetch(i).wait()
        rows = stage[lax.rem(i, 2)]
        for c in range(n_col):
            table[pl.ds(i * (STAGE_ROWS * n_col) + c, STAGE_ROWS, stride=n_col), :] = rows[:, c * LANES:(c + 1) * LANES].astype(F32)

    table[pl.ds(n_rows * n_col, 8), :] = jnp.zeros((8, LANES), F32)


def row_slice(i, n_col):
    return pl.ds(pl.multiple_of(i * n_col, n_col), n_col)


def list_base(p, e, n_local):
    return (p * n_local + e) * LIST


def tile_rows(buf, r0, n_rows, n_col):
    return jnp.concatenate([buf[pl.ds(r0 * n_col + c, n_rows, stride=n_col), :] for c in range(n_col)], axis=1)


def put_rows(buf, r0, rows, n_col):
    for c in range(n_col):
        buf[pl.ds(r0 * n_col + c, rows.shape[0], stride=n_col), :] = rows[:, c * LANES:(c + 1) * LANES]


def for_lists(tok, e, n_src, n_local, step, unroll):
    row = jnp.int32(0)
    for p in range(n_src):
        base = list_base(p, e, n_local)
        cnt = tok[base + LIST - 1]

        def group(i, _, base=base, row=row):
            step(base + i * unroll, row + i * unroll)
            return 0

        lax.fori_loop(0, lax.div(cnt + (unroll - 1), unroll), group, 0)
        row = row + cnt
    return row


def for_tiles(total, tile):
    n_full = lax.div(total + (TILE // 2 - 1), TILE)

    @pl.loop(0, n_full)
    def _(i):
        tile(i * TILE, TILE)

    @pl.when(total > n_full * TILE)
    def _():
        tile(n_full * TILE, TILE // 2)


def add_rows(tok, g, acc, buf, e, n_src, n_local, n_col):
    def step(pos, row):
        toks = [tok[pos + k] for k in range(8)]
        rows = [buf[row_slice(row + k, n_col), :] for k in range(8)]
        if g is not None:
            rows = [r * g[pos + k] for k, r in enumerate(rows)]
        sums = [acc[row_slice(t, n_col), :] + r for t, r in zip(toks, rows)]
        for t, s in zip(toks, sums):
            acc[row_slice(t, n_col), :] = s

    for_lists(tok, e, n_src, n_local, step, 8)


def forward_kernel(n_src, n_local, n_rows, n_col, tok, g, x_hbm, w_one, w_three, w_two, y_hbm, table, acc, buf, stage, sem):
    e = pl.program_id(0)

    @pl.when(e == 0)
    def _():
        acc[...] = jnp.zeros_like(acc)
        buf[...] = jnp.zeros_like(buf)
        load_table(x_hbm, table, stage, sem, n_rows, n_col)

    def pick(pos, row):
        rows = [table[row_slice(tok[pos + k], n_col), :] for k in range(8)]
        for k in range(8):
            buf[row_slice(row + k, n_col), :] = rows[k]

    total = for_lists(tok, e, n_src, n_local, pick, 8)

    def tile(r0, m):
        x = tile_rows(buf, r0, m, n_col).astype(BF16)
        pre_one = dot_nn(x, w_one[0])
        pre_three = dot_nn(x, w_three[0])
        hidden = (pre_one * jax.nn.sigmoid(pre_one) * pre_three).astype(BF16)
        put_rows(buf, r0, dot_nn(hidden, w_two[0]).astype(BF16).astype(F32), n_col)

    for_tiles(total, tile)
    add_rows(tok, g, acc, buf, e, n_src, n_local, n_col)

    @pl.when(e == n_local - 1)
    def _():
        out = pltpu.make_async_copy(acc.at[pl.ds(0, n_rows * n_col)], y_hbm, sem.at[0])
        out.start()
        out.wait()


def buf_rows(n_src):
    return n_src * PER_SRC + 8


def forward_partial(tok, g, x_all, w_one, w_three, w_two):
    n_rows, model = x_all.shape
    n_local, _, ffn = w_one.shape
    n_src = tok.shape[0] // (n_local * LIST)
    n_col = model // LANES
    smem = pl.BlockSpec(memory_space=pltpu.SMEM)
    hbm = pl.BlockSpec(memory_space=pl.ANY)
    per_expert = lambda a, b: pl.BlockSpec((1, a, b), lambda e: (e, 0, 0))
    pairs = n_rows * 8 // n_src
    return pl.pallas_call(
        functools.partial(forward_kernel, n_src, n_local, n_rows, n_col),
        out_shape=jax.ShapeDtypeStruct((n_rows * n_col, LANES), F32),
        grid=(n_local,),
        in_specs=[smem, smem, hbm, per_expert(model, ffn), per_expert(model, ffn), per_expert(ffn, model)],
        out_specs=hbm,
        scratch_shapes=[
            pltpu.VMEM((n_rows * n_col + 8, LANES), F32),
            pltpu.VMEM((n_rows * n_col + 8, LANES), F32),
            pltpu.VMEM((buf_rows(n_src) * n_col, LANES), F32),
            pltpu.VMEM((2, STAGE_ROWS, model), BF16),
            pltpu.SemaphoreType.DMA((2,)),
        ],
        compiler_params=pltpu.CompilerParams(dimension_semantics=('arbitrary',), vmem_limit_bytes=VMEM_LIMIT),
        cost_estimate=pl.CostEstimate(flops=6 * pairs * model * ffn, bytes_accessed=6 * n_local * model * ffn, transcendentals=0),
        name='forward_partial',
    )(tok, g, x_all, w_one, w_three, w_two)


def pick_kernel(n_src, n_local, n_rows, n_col, tok, g, x_hbm, dy_hbm, x_out, d_out, x_table, d_table, x_buf, d_buf, stage, sem):
    e = pl.program_id(0)

    @pl.when(e == 0)
    def _():
        load_table(x_hbm, x_table, stage, sem, n_rows, n_col)
        load_table(dy_hbm, d_table, stage, sem, n_rows, n_col)

    def pick(pos, row):
        toks = [tok[pos + k] for k in range(8)]
        x_rows = [x_table[row_slice(t, n_col), :] for t in toks]
        d_rows = [d_table[row_slice(t, n_col), :] * g[pos + k] for k, t in enumerate(toks)]
        for k in range(8):
            x_buf[row_slice(row + k, n_col), :] = x_rows[k]
            d_buf[row_slice(row + k, n_col), :] = d_rows[k]

    total = for_lists(tok, e, n_src, n_local, pick, 8)

    @pl.loop(0, lax.div(total + (TILE - 1), TILE))
    def _(i):
        r0 = pl.multiple_of(i * TILE, TILE)
        used = lax.broadcasted_iota(jnp.int32, (TILE, n_col * LANES), 0) < total - r0
        x_out[0, pl.ds(r0, TILE), :] = jnp.where(used, tile_rows(x_buf, r0, TILE, n_col), 0.0).astype(BF16)
        d_out[0, pl.ds(r0, TILE), :] = jnp.where(used, tile_rows(d_buf, r0, TILE, n_col), 0.0).astype(BF16)


def pick_rows(tok, g, x_all, dy_all, n_local):
    n_rows, model = x_all.shape
    n_src = tok.shape[0] // (n_local * LIST)
    n_col = model // LANES
    cap = n_src * PER_SRC
    smem = pl.BlockSpec(memory_space=pltpu.SMEM)
    hbm = pl.BlockSpec(memory_space=pl.ANY)
    table = pltpu.VMEM((n_rows * n_col + 8, LANES), F32)
    buf = pltpu.VMEM((buf_rows(n_src) * n_col, LANES), F32)
    rows_out = jax.ShapeDtypeStruct((n_local, cap, model), BF16)
    rows_spec = pl.BlockSpec((1, cap, model), lambda e: (e, 0, 0))
    return pl.pallas_call(
        functools.partial(pick_kernel, n_src, n_local, n_rows, n_col),
        out_shape=(rows_out, rows_out),
        grid=(n_local,),
        in_specs=[smem, smem, hbm, hbm],
        out_specs=(rows_spec, rows_spec),
        scratch_shapes=[table, table, buf, buf, pltpu.VMEM((2, STAGE_ROWS, model), BF16), pltpu.SemaphoreType.DMA((2,))],
        compiler_params=pltpu.CompilerParams(dimension_semantics=('arbitrary',), vmem_limit_bytes=VMEM_LIMIT),
        cost_estimate=pl.CostEstimate(flops=40 * 10**9, bytes_accessed=4 * n_local * cap * model, transcendentals=0),
        name='pick_rows',
    )(tok, g, x_all, dy_all)


def list_total(tok, e, n_src, n_local):
    total = tok[list_base(0, e, n_local) + LIST - 1]
    for p in range(1, n_src):
        total = total + tok[list_base(p, e, n_local) + LIST - 1]
    return total


def backward_kernel(n_src, n_local, n_rows, n_col, tok, x_ref, d_ref, w_one, w_three, w_two, dx_hbm, h_ref, d1_ref, d3_ref, acc, buf, sem):
    e = pl.program_id(0)

    @pl.when(e == 0)
    def _():
        acc[...] = jnp.zeros_like(acc)
        buf[...] = jnp.zeros_like(buf)

    def tile(r0, m):
        rows = pl.ds(pl.multiple_of(r0, TILE // 2), m)
        x = x_ref[0, rows, :]
        pre_one = dot_nn(x, w_one[0])
        pre_three = dot_nn(x, w_three[0])
        d_hidden = dot_nt(d_ref[0, rows, :], w_two[0]).astype(BF16).astype(F32)
        sig_one = jax.nn.sigmoid(pre_one)
        act_one = pre_one * sig_one
        h_ref[0, rows, :] = (act_one * pre_three).astype(BF16)
        d_three = (d_hidden * act_one).astype(BF16)
        d_one = (d_hidden * pre_three * sig_one * (1.0 + pre_one * (1.0 - sig_one))).astype(BF16)
        d1_ref[0, rows, :] = d_one
        d3_ref[0, rows, :] = d_three
        dx = dot_nt(d_one, w_one[0]) + dot_nt(d_three, w_three[0])
        put_rows(buf, r0, dx.astype(BF16).astype(F32), n_col)
        if m < TILE:
            rest = pl.ds(pl.multiple_of(r0 + m, TILE // 2), TILE - m)
            for ref in (h_ref, d1_ref, d3_ref):
                ref[0, rest, :] = jnp.zeros((TILE - m, ref.shape[2]), BF16)

    for_tiles(list_total(tok, e, n_src, n_local), tile)
    add_rows(tok, None, acc, buf, e, n_src, n_local, n_col)

    @pl.when(e == n_local - 1)
    def _():
        out = pltpu.make_async_copy(acc.at[pl.ds(0, n_rows * n_col)], dx_hbm, sem)
        out.start()
        out.wait()


def backward_partial(tok, x_rows, d_rows, w_one, w_three, w_two, n_rows):
    n_local, cap, model = x_rows.shape
    ffn = w_one.shape[2]
    n_src = cap // PER_SRC
    n_col = model // LANES
    smem = pl.BlockSpec(memory_space=pltpu.SMEM)
    hbm = pl.BlockSpec(memory_space=pl.ANY)
    per_expert = lambda a, b: pl.BlockSpec((1, a, b), lambda e: (e, 0, 0))
    ffn_out = jax.ShapeDtypeStruct((n_local, cap, ffn), BF16)
    pairs = n_rows * 8 // n_src
    return pl.pallas_call(
        functools.partial(backward_kernel, n_src, n_local, n_rows, n_col),
        out_shape=(jax.ShapeDtypeStruct((n_rows * n_col, LANES), F32), ffn_out, ffn_out, ffn_out),
        grid=(n_local,),
        in_specs=[smem, per_expert(cap, model), per_expert(cap, model), per_expert(model, ffn), per_expert(model, ffn), per_expert(ffn, model)],
        out_specs=(hbm, per_expert(cap, ffn), per_expert(cap, ffn), per_expert(cap, ffn)),
        scratch_shapes=[
            pltpu.VMEM((n_rows * n_col + 8, LANES), F32),
            pltpu.VMEM((buf_rows(n_src) * n_col, LANES), F32),
            pltpu.SemaphoreType.DMA,
        ],
        compiler_params=pltpu.CompilerParams(dimension_semantics=('arbitrary',), vmem_limit_bytes=VMEM_LIMIT),
        cost_estimate=pl.CostEstimate(flops=10 * pairs * model * ffn, bytes_accessed=6 * n_local * cap * ffn, transcendentals=0),
        name='backward_partial',
    )(tok, x_rows, d_rows, w_one, w_three, w_two)


def grad_kernel(n_src, n_local, tok, x_ref, d_ref, h_ref, d1_ref, d3_ref, g1_ref, g3_ref, g2_ref):
    total = list_total(tok, pl.program_id(0), n_src, n_local)
    used = lax.div(total + (TILE - 1), TILE)
    for n in range(1, n_src * PER_SRC // TILE + 1):
        @pl.when(used == n)
        def _(n=n):
            rows = pl.ds(0, n * TILE)
            g1_ref[0] = dot_tn(x_ref[0, rows, :], d1_ref[0, rows, :]).astype(BF16)
            g3_ref[0] = dot_tn(x_ref[0, rows, :], d3_ref[0, rows, :]).astype(BF16)
            g2_ref[0] = dot_tn(h_ref[0, rows, :], d_ref[0, rows, :]).astype(BF16)


def weight_grads(tok, x_rows, d_rows, hidden, d_one, d_three):
    n_local, cap, model = x_rows.shape
    ffn = hidden.shape[2]
    n_src = cap // PER_SRC
    per_expert = lambda a, b: pl.BlockSpec((1, a, b), lambda e: (e, 0, 0))
    in_grad = jax.ShapeDtypeStruct((n_local, model, ffn), BF16)
    pairs = n_local * cap // 2
    return pl.pallas_call(
        functools.partial(grad_kernel, n_src, n_local),
        out_shape=(in_grad, in_grad, jax.ShapeDtypeStruct((n_local, ffn, model), BF16)),
        grid=(n_local,),
        in_specs=[pl.BlockSpec(memory_space=pltpu.SMEM), per_expert(cap, model), per_expert(cap, model), per_expert(cap, ffn), per_expert(cap, ffn), per_expert(cap, ffn)],
        out_specs=(per_expert(model, ffn), per_expert(model, ffn), per_expert(ffn, model)),
        compiler_params=pltpu.CompilerParams(dimension_semantics=('arbitrary',), vmem_limit_bytes=VMEM_LIMIT),
        cost_estimate=pl.CostEstimate(flops=6 * pairs * model * ffn, bytes_accessed=6 * n_local * cap * ffn, transcendentals=0),
        name='weight_grads',
    )(tok, x_rows, d_rows, hidden, d_one, d_three)


def solution(mesh):
    n_stage = mesh.shape['stage']
    n_dev = mesh.shape['expert']
    to_next = [(stage_idx, (stage_idx + 1) % n_stage) for stage_idx in range(n_stage)]
    to_prev = [((stage_idx + 1) % n_stage, stage_idx) for stage_idx in range(n_stage)]
    tok_spec = P('stage', 'expert', None)
    w_spec = P('stage', 'expert', None, None)

    def moe_body(x_act, route_idx, route_wts, w_one, w_three, w_two, dy_act):
        n_tok, model_dim = x_act.shape[1:]
        n_local = w_one.shape[1]
        n_exp = n_local * n_dev
        n_rows = n_tok * n_dev
        w_in_one, w_in_three, w_out = w_one[0], w_three[0], w_two[0]

        def gather_tokens(rows):
            return lax.all_gather(rows, 'expert', axis=0, tiled=True)

        def scatter_sums(partial):
            own = lax.psum_scatter(partial, 'expert', scatter_dimension=0, tiled=True)
            return own.reshape(n_tok, model_dim).astype(BF16)

        x_dst = lax.ppermute(x_act[0], 'stage', to_next)
        idx_dst = lax.ppermute(route_idx[0], 'stage', to_next)
        wts_dst = lax.ppermute(route_wts[0], 'stage', to_next)
        x_dst, idx_dst, wts_dst, x_again, dy_src = lax.optimization_barrier((x_dst, idx_dst, wts_dst, x_act[0], dy_act[0]))
        x_all = gather_tokens(x_dst)
        x_dst_again = lax.ppermute(x_again, 'stage', to_next)
        tok_own, g_own = route_lists(idx_dst, wts_dst, lax.axis_index('expert') * n_tok, n_exp, n_rows)
        n_list = n_local * LIST
        lists = jnp.concatenate([tok_own.reshape(n_dev, n_list).astype(F32), g_own.reshape(n_dev, n_list)], axis=1)
        lists = lax.all_to_all(lists, 'expert', 0, 0, tiled=True)
        lists, x_dst_again, dy_src, x_all = lax.optimization_barrier((lists, x_dst_again, dy_src, x_all))
        tok = lists[:, :n_list].astype(jnp.int32).reshape(n_dev * n_list)
        g = lists[:, n_list:].reshape(n_dev * n_list)
        dy_all = gather_tokens(dy_src)
        x_all_again = gather_tokens(x_dst_again)

        y_sum = forward_partial(tok, g, x_all, w_in_one, w_in_three, w_out)
        y_sum, x_all_again, dy_all = lax.optimization_barrier((y_sum, x_all_again, dy_all))
        y_dst = scatter_sums(y_sum)

        x_rows, d_rows = pick_rows(tok, g, x_all_again, dy_all, n_local)
        dx_sum, hidden, d_one, d_three = backward_partial(tok, x_rows, d_rows, w_in_one, w_in_three, w_out, n_rows)
        dx_dst = scatter_sums(dx_sum)
        dx_src = lax.ppermute(dx_dst, 'stage', to_prev)
        g_one, g_three, g_two = weight_grads(tok, x_rows, d_rows, hidden, d_one, d_three)
        return y_dst[None], dx_src[None], g_one[None], g_three[None], g_two[None]

    return jax.shard_map(moe_body, mesh=mesh, in_specs=(tok_spec, tok_spec, tok_spec, w_spec, w_spec, w_spec, tok_spec), out_specs=(tok_spec, tok_spec, w_spec, w_spec, w_spec), check_vma=False)
```

```python
import functools

import jax
import jax.numpy as jnp
from jax import lax
from jax.experimental import pallas as pl
from jax.experimental.pallas import tpu as pltpu
from jax.sharding import PartitionSpec as P


F32 = jnp.float32
BF16 = jnp.bfloat16
LIST = 264
GROUP = 8
PER_SRC = 256
TILE = 256
TILE_GROUPS = TILE // GROUP
LANES = 128
STAGE_ROWS = 256
VMEM_LIMIT = 66 * 1000 * 1000


def dot_nn(a, b):
    return lax.dot_general(a, b, (((1,), (0,)), ((), ())), preferred_element_type=F32)


def dot_nt(a, b):
    return lax.dot_general(a, b, (((1,), (1,)), ((), ())), preferred_element_type=F32)


def dot_tn(a, b):
    return lax.dot_general(a, b, (((0,), (0,)), ((), ())), preferred_element_type=F32)


def route_kernel(n_tok, top_k, n_local, n_dev, n_col, base_ref, idx_ref, wts_ref, out_ref, ptr_ref):
    n_list = n_local * LIST
    base = base_ref[0]
    dummy = float(n_tok * n_dev * n_col)

    def first(e):
        return lax.div(e, n_local) * (2 * n_list) + lax.rem(e, n_local) * LIST

    @pl.loop(0, n_local * n_dev)
    def _(e):
        ptr_ref[e] = first(e)

    @pl.loop(0, n_tok // 2)
    def _(i):
        at = i * (2 * top_k)
        experts = [idx_ref[at + j] for j in range(2 * top_k)]
        wts = [wts_ref[at + j] for j in range(2 * top_k)]
        for k in range(2):
            row = ((base + 2 * i + k) * n_col).astype(F32)
            part = slice(k * top_k, (k + 1) * top_k)
            ptrs = [ptr_ref[e] for e in experts[part]]
            for e, p, w in zip(experts[part], ptrs, wts[part]):
                out_ref[p] = row
                out_ref[p + n_list] = w
                ptr_ref[e] = p + 1

    @pl.loop(0, n_local * n_dev)
    def _(e):
        p = ptr_ref[e]
        for k in range(GROUP - 1):
            out_ref[p + k] = dummy
            out_ref[p + k + n_list] = 0.0
        out_ref[first(e) + LIST - 1] = (p - first(e)).astype(F32)


def route_lists(idx, wts, base, n_local, n_dev, n_col):
    n_tok, top_k = idx.shape
    smem = pl.BlockSpec(memory_space=pltpu.SMEM)
    return pl.pallas_call(
        functools.partial(route_kernel, n_tok, top_k, n_local, n_dev, n_col),
        out_shape=jax.ShapeDtypeStruct((n_dev * 2 * n_local * LIST,), F32),
        in_specs=[smem, smem, smem],
        out_specs=smem,
        scratch_shapes=[pltpu.SMEM((n_local * n_dev,), jnp.int32)],
        cost_estimate=pl.CostEstimate(flops=60 * 10**8, bytes_accessed=8 * n_local * n_dev * LIST, transcendentals=0),
        name='route_lists',
    )(base.reshape(1), idx.reshape(n_tok * top_k), wts.reshape(n_tok * top_k))


def load_table(src_hbm, table, stage, sem, n_rows, n_col):
    n_chunk = n_rows // STAGE_ROWS

    def fetch(i):
        slot = lax.rem(i, 2)
        return pltpu.make_async_copy(src_hbm.at[pl.ds(pl.multiple_of(i * STAGE_ROWS, STAGE_ROWS), STAGE_ROWS)], stage.at[slot], sem.at[slot])

    fetch(0).start()

    @pl.loop(0, n_chunk)
    def _(i):
        @pl.when(i + 1 < n_chunk)
        def _():
            fetch(i + 1).start()

        fetch(i).wait()
        rows = stage[lax.rem(i, 2)]
        for c in range(n_col):
            table[pl.ds(i * (STAGE_ROWS * n_col) + c, STAGE_ROWS, stride=n_col), :] = rows[:, c * LANES:(c + 1) * LANES].astype(F32)

    table[pl.ds(n_rows * n_col, 8), :] = jnp.zeros((8, LANES), F32)


SLOT = 4 * (PER_SRC // GROUP) + TILE_GROUPS + 16


def rows_at(first, n_col):
    return pl.ds(pl.multiple_of(first, n_col), n_col)


def n_groups(tok, p, e, n_local):
    return lax.div(tok[(p * n_local + e) * LIST + LIST - 1] + (GROUP - 1), GROUP)


def n_tiles(tok, e, n_src, n_local):
    groups = n_groups(tok, 0, e, n_local)
    for p in range(1, n_src):
        groups = groups + n_groups(tok, p, e, n_local)
    return lax.div(groups + (TILE_GROUPS - 1), TILE_GROUPS)


def list_groups(tok, grp, e, n_src, n_local):
    empty = n_src * n_local * LIST
    at = lax.rem(e, 3) * SLOT
    for p in range(n_src):
        base = (p * n_local + e) * LIST
        groups = n_groups(tok, p, e, n_local)

        @pl.loop(0, lax.div(groups + 3, 4))
        def _(i, base=base, at=at):
            for k in range(4):
                grp[at + 4 * i + k] = base + (4 * i + k) * GROUP

        at = at + groups
    for k in range(TILE_GROUPS):
        grp[at + k] = empty


def start_groups(tok, grp, n_src, n_local):
    for k in range(TILE_GROUPS):
        grp[3 * SLOT + k] = n_src * n_local * LIST
    list_groups(tok, grp, jnp.int32(0), n_src, n_local)


def pick_group(tok, g, tables, bufs, base, row, n_col):
    for k in range(GROUP):
        src = rows_at(tok[base + k], n_col)
        dst = pl.ds(row * n_col + k * n_col, n_col)
        bufs[0][dst, :] = tables[0][src, :]
        if len(tables) > 1:
            bufs[1][dst, :] = tables[1][src, :] * g[base + k]


def add_groups(tok, g, acc, buf, bases, row, n_col):
    dsts, rows = [], []
    for q, base in enumerate(bases):
        for k in range(GROUP):
            dsts.append(rows_at(tok[base + k], n_col))
            val = buf[pl.ds((row + q * GROUP + k) * n_col, n_col), :]
            rows.append(val if g is None else val * g[base + k])
    sums = [acc[d, :] + r for d, r in zip(dsts, rows)]
    for d, r in zip(dsts, sums):
        acc[d, :] = r


def tile_rows(buf, n_col):
    return jnp.concatenate([buf[pl.ds(c, TILE, stride=n_col), :] for c in range(n_col)], axis=1).astype(BF16)


def put_rows(buf, rows, n_col):
    for c in range(n_col):
        buf[pl.ds(c, TILE, stride=n_col), :] = rows[:, c * LANES:(c + 1) * LANES].astype(F32)


def pipelined_tiles(e, n_src, n_local, n_col, tok, g, grp, prev, tables, pick_bufs, acc, out_buf, compute):
    tiles = n_tiles(tok, e, n_src, n_local)
    here = lax.rem(e, 3) * SLOT
    following = lax.rem(e + 1, 3) * SLOT

    @pl.when(e == 0)
    def _():
        prev[0] = 3 * SLOT
        start_groups(tok, grp, n_src, n_local)

        @pl.loop(0, TILE_GROUPS)
        def _(q):
            pick_group(tok, g, tables, pick_bufs, grp[q], pl.multiple_of(q * GROUP, GROUP), n_col)

    list_groups(tok, grp, lax.min(e + 1, n_local - 1), n_src, n_local)

    @pl.loop(0, tiles)
    def _(i):
        last = prev[0]
        coming = jnp.where(i + 1 < tiles, here + (i + 1) * TILE_GROUPS, following)

        def side(part, parts):
            per = TILE_GROUPS // parts
            for q in range(part * per, (part + 1) * per, 2):
                add_groups(tok, g, acc, out_buf, [grp[last + q], grp[last + q + 1]], q * GROUP, n_col)
                for r in (q, q + 1):
                    pick_group(tok, g, tables, pick_bufs, grp[coming + r], r * GROUP, n_col)

        compute(i, side)
        prev[0] = here + i * TILE_GROUPS

    @pl.when(e == n_local - 1)
    def _():
        @pl.loop(0, TILE_GROUPS)
        def _(q):
            add_groups(tok, g, acc, out_buf, [grp[prev[0] + q]], pl.multiple_of(q * GROUP, GROUP), n_col)


def forward_kernel(n_src, n_local, n_rows, n_col, tok, g, x_hbm, dy_hbm, w_one, w_three, w_two, y_hbm, d_ref, x_table, d_table, acc, x_buf, d_buf, out_buf, stage, grp, prev, sem):
    e = pl.program_id(0)

    @pl.when(e == 0)
    def _():
        acc[...] = jnp.zeros_like(acc)
        load_table(x_hbm, x_table, stage, sem, n_rows, n_col)
        load_table(dy_hbm, d_table, stage, sem, n_rows, n_col)

    def compute(i, side):
        rows = pl.ds(pl.multiple_of(i * TILE, TILE), TILE)
        x = tile_rows(x_buf, n_col)
        d_ref[0, rows, :] = tile_rows(d_buf, n_col)
        side(0, 4)
        pre_one = dot_nn(x, w_one[0])
        side(1, 4)
        pre_three = dot_nn(x, w_three[0])
        side(2, 4)
        hidden = (pre_one * jax.nn.sigmoid(pre_one) * pre_three).astype(BF16)
        side(3, 4)
        put_rows(out_buf, dot_nn(hidden, w_two[0]).astype(BF16), n_col)

    pipelined_tiles(e, n_src, n_local, n_col, tok, g, grp, prev, (x_table, d_table), (x_buf, d_buf), acc, out_buf, compute)

    @pl.when(e == n_local - 1)
    def _():
        out = pltpu.make_async_copy(acc.at[pl.ds(0, n_rows * n_col)], y_hbm, sem.at[0])
        out.start()
        out.wait()


def kernel_scratch(n_rows, model, n_table, n_pick):
    n_col = model // LANES
    table = pltpu.VMEM((n_rows * n_col + 8, LANES), F32)
    tile = pltpu.VMEM((TILE * n_col, LANES), F32)
    return [table] * (n_table + 1) + [tile] * (n_pick + 1) + [
        pltpu.VMEM((2, STAGE_ROWS, model), BF16),
        pltpu.SMEM((3 * SLOT + TILE_GROUPS,), jnp.int32),
        pltpu.SMEM((1,), jnp.int32),
        pltpu.SemaphoreType.DMA((2,)),
    ]


def per_expert(a, b):
    return pl.BlockSpec((1, a, b), lambda e: (e, 0, 0))


def forward_partial(tok, g, x_all, dy_all, w_one, w_three, w_two, n_src):
    n_rows, model = x_all.shape
    n_local, _, ffn = w_one.shape
    n_col = model // LANES
    cap = n_src * PER_SRC
    smem = pl.BlockSpec(memory_space=pltpu.SMEM)
    hbm = pl.BlockSpec(memory_space=pl.ANY)
    pairs = n_rows * 8 // n_src
    return pl.pallas_call(
        functools.partial(forward_kernel, n_src, n_local, n_rows, n_col),
        out_shape=(jax.ShapeDtypeStruct((n_rows * n_col, LANES), F32), jax.ShapeDtypeStruct((n_local, cap, model), BF16)),
        grid=(n_local,),
        in_specs=[smem, smem, hbm, hbm, per_expert(model, ffn), per_expert(model, ffn), per_expert(ffn, model)],
        out_specs=(hbm, per_expert(cap, model)),
        scratch_shapes=kernel_scratch(n_rows, model, 2, 2),
        compiler_params=pltpu.CompilerParams(dimension_semantics=('arbitrary',), vmem_limit_bytes=VMEM_LIMIT),
        cost_estimate=pl.CostEstimate(flops=6 * pairs * model * ffn, bytes_accessed=6 * n_local * model * ffn, transcendentals=0),
        name='forward_partial',
    )(tok, g, x_all, dy_all, w_one, w_three, w_two)


def backward_kernel(n_src, n_local, n_rows, n_col, n_part, tok, x_hbm, d_ref, w_one, w_three, w_two, *rest):
    parts, rest = rest[:n_part], rest[n_part:]
    x_ref, h_ref, d1_ref, d3_ref, table, acc, x_buf, out_buf, stage, grp, prev, sem = rest
    e = pl.program_id(0)

    @pl.when(e == 0)
    def _():
        acc[...] = jnp.zeros_like(acc)
        load_table(x_hbm, table, stage, sem, n_rows, n_col)

    def compute(i, side):
        rows = pl.ds(pl.multiple_of(i * TILE, TILE), TILE)
        x = tile_rows(x_buf, n_col)
        x_ref[0, rows, :] = x
        side(0, 4)
        pre_one = dot_nn(x, w_one[0])
        side(1, 4)
        pre_three = dot_nn(x, w_three[0])
        side(2, 4)
        d_hidden = dot_nt(d_ref[0, rows, :], w_two[0]).astype(BF16).astype(F32)
        side(3, 4)
        sig_one = jax.nn.sigmoid(pre_one)
        act_one = pre_one * sig_one
        h_ref[0, rows, :] = (act_one * pre_three).astype(BF16)
        d_three = (d_hidden * act_one).astype(BF16)
        d_one = (d_hidden * pre_three * sig_one * (1.0 + pre_one * (1.0 - sig_one))).astype(BF16)
        d1_ref[0, rows, :] = d_one
        d3_ref[0, rows, :] = d_three
        dx = dot_nt(d_one, w_one[0]) + dot_nt(d_three, w_three[0])
        put_rows(out_buf, dx.astype(BF16), n_col)

    pipelined_tiles(e, n_src, n_local, n_col, tok, None, grp, prev, (table,), (x_buf,), acc, out_buf, compute)

    @pl.when(e == n_local - 1)
    def _():
        own = n_rows * n_col // n_src
        part = own // n_part
        outs = [
            pltpu.make_async_copy(acc.at[pl.ds(q * own + k * part, part)], parts[k].at[pl.ds(q * part, part)], sem.at[0])
            for k in range(n_part) for q in range(n_src)
        ]
        for out in outs:
            out.start()
        for out in outs:
            out.wait()


def backward_partial(tok, x_all, d_rows, w_one, w_three, w_two, n_src, n_part):
    n_rows, model = x_all.shape
    n_local, cap, _ = d_rows.shape
    ffn = w_one.shape[2]
    n_col = model // LANES
    smem = pl.BlockSpec(memory_space=pltpu.SMEM)
    hbm = pl.BlockSpec(memory_space=pl.ANY)
    ffn_out = jax.ShapeDtypeStruct((n_local, cap, ffn), BF16)
    pairs = n_rows * 8 // n_src
    outs = pl.pallas_call(
        functools.partial(backward_kernel, n_src, n_local, n_rows, n_col, n_part),
        out_shape=(jax.ShapeDtypeStruct((n_rows * n_col // n_part, LANES), F32),) * n_part + (jax.ShapeDtypeStruct((n_local, cap, model), BF16), ffn_out, ffn_out, ffn_out),
        grid=(n_local,),
        in_specs=[smem, hbm, per_expert(cap, model), per_expert(model, ffn), per_expert(model, ffn), per_expert(ffn, model)],
        out_specs=(hbm,) * n_part + (per_expert(cap, model), per_expert(cap, ffn), per_expert(cap, ffn), per_expert(cap, ffn)),
        scratch_shapes=kernel_scratch(n_rows, model, 1, 1),
        compiler_params=pltpu.CompilerParams(dimension_semantics=('arbitrary',), vmem_limit_bytes=VMEM_LIMIT),
        cost_estimate=pl.CostEstimate(flops=10 * pairs * model * ffn, bytes_accessed=6 * n_local * cap * ffn, transcendentals=0),
        name='backward_partial',
    )(tok, x_all, d_rows, w_one, w_three, w_two)
    return outs[:n_part], outs[n_part:]


def grad_kernel(n_src, n_local, first, tok, x_ref, d_ref, h_ref, d1_ref, d3_ref, *refs):
    g1_ref, g3_ref, g2_ref = refs[-3:]
    used = n_tiles(tok, pl.program_id(0) + first, n_src, n_local)
    for n in range(1, n_src * PER_SRC // TILE + 1):
        @pl.when(used == n)
        def _(n=n):
            rows = pl.ds(0, n * TILE)
            g1_ref[0] = dot_tn(x_ref[0, rows, :], d1_ref[0, rows, :]).astype(BF16)
            g3_ref[0] = dot_tn(x_ref[0, rows, :], d3_ref[0, rows, :]).astype(BF16)
            g2_ref[0] = dot_tn(h_ref[0, rows, :], d_ref[0, rows, :]).astype(BF16)


def weight_grads(tok, x_rows, d_rows, hidden, d_one, d_three, n_src, first, count, so_far):
    n_local, cap, model = x_rows.shape
    ffn = hidden.shape[2]
    block = lambda a, b: pl.BlockSpec((1, a, b), lambda e: (e + first, 0, 0))
    in_grad = jax.ShapeDtypeStruct((n_local, model, ffn), BF16)
    pairs = count * cap // 2
    return pl.pallas_call(
        functools.partial(grad_kernel, n_src, n_local, first),
        out_shape=(in_grad, in_grad, jax.ShapeDtypeStruct((n_local, ffn, model), BF16)),
        grid=(count,),
        in_specs=[pl.BlockSpec(memory_space=pltpu.SMEM), block(cap, model), block(cap, model), block(cap, ffn), block(cap, ffn), block(cap, ffn)] + [pl.BlockSpec(memory_space=pl.ANY)] * len(so_far),
        out_specs=(block(model, ffn), block(model, ffn), block(ffn, model)),
        input_output_aliases={6 + k: k for k in range(len(so_far))},
        compiler_params=pltpu.CompilerParams(dimension_semantics=('arbitrary',), vmem_limit_bytes=VMEM_LIMIT),
        cost_estimate=pl.CostEstimate(flops=6 * pairs * model * ffn, bytes_accessed=6 * count * cap * ffn, transcendentals=0),
        name='weight_grads',
    )(tok, x_rows, d_rows, hidden, d_one, d_three, *so_far)


def solution(mesh):
    n_stage = mesh.shape['stage']
    n_dev = mesh.shape['expert']
    to_next = [(stage_idx, (stage_idx + 1) % n_stage) for stage_idx in range(n_stage)]
    to_prev = [((stage_idx + 1) % n_stage, stage_idx) for stage_idx in range(n_stage)]
    tok_spec = P('stage', 'expert', None)
    w_spec = P('stage', 'expert', None, None)

    def moe_body(x_act, route_idx, route_wts, w_one, w_three, w_two, dy_act):
        n_tok, model_dim = x_act.shape[1:]
        n_local = w_one.shape[1]
        n_rows = n_tok * n_dev
        n_col = model_dim // LANES
        w_in_one, w_in_three, w_out = w_one[0], w_three[0], w_two[0]

        def gather_tokens(rows):
            return lax.all_gather(rows, 'expert', axis=0, tiled=True)

        def scatter_sums(partial):
            own = lax.psum_scatter(partial, 'expert', scatter_dimension=0, tiled=True)
            return own.reshape(-1, model_dim).astype(BF16)

        x_dst = lax.ppermute(x_act[0], 'stage', to_next)
        idx_dst = lax.ppermute(route_idx[0], 'stage', to_next)
        wts_dst = lax.ppermute(route_wts[0], 'stage', to_next)
        dy_all = gather_tokens(dy_act[0])
        x_dst, idx_dst, wts_dst, x_again = lax.optimization_barrier((x_dst, idx_dst, wts_dst, x_act[0]))
        x_all = gather_tokens(x_dst)
        x_dst_again = lax.ppermute(x_again, 'stage', to_next)
        lists = route_lists(idx_dst, wts_dst, lax.axis_index('expert') * n_tok, n_local, n_dev, n_col)
        n_list = n_local * LIST
        lists = lax.all_to_all(lists.reshape(n_dev, 2 * n_list), 'expert', 0, 0, tiled=True)
        lists, x_dst_again, dy_all, x_all = lax.optimization_barrier((lists, x_dst_again, dy_all, x_all))
        tok = jnp.concatenate([lists[:, :n_list].astype(jnp.int32).reshape(n_dev * n_list), jnp.full((LANES,), n_rows * n_col, jnp.int32)])
        g = jnp.concatenate([lists[:, n_list:].reshape(n_dev * n_list), jnp.zeros((LANES,), F32)])
        x_all_again = gather_tokens(x_dst_again)

        y_sum, d_rows = forward_partial(tok, g, x_all, dy_all, w_in_one, w_in_three, w_out, n_dev)
        y_sum, x_all_again, d_rows = lax.optimization_barrier((y_sum, x_all_again, d_rows))
        y_dst = scatter_sums(y_sum)

        (dx_low, dx_high), (x_rows, hidden, d_one, d_three) = backward_partial(tok, x_all_again, d_rows, w_in_one, w_in_three, w_out, n_dev, 2)
        dx_low = scatter_sums(dx_low)
        dx_high = scatter_sums(dx_high)
        dx_low = lax.ppermute(dx_low, 'stage', to_prev)
        dx_high = lax.ppermute(dx_high, 'stage', to_prev)
        early = n_local * 5 // 8
        grads = weight_grads(tok, x_rows, d_rows, hidden, d_one, d_three, n_dev, 0, early, ())
        g_one, g_three, g_two = weight_grads(tok, x_rows, d_rows, hidden, d_one, d_three, n_dev, early, n_local - early, grads)
        dx_src = jnp.concatenate([dx_low, dx_high])
        return y_dst[None], dx_src[None], g_one[None], g_three[None], g_two[None]

    return jax.shard_map(moe_body, mesh=mesh, in_specs=(tok_spec, tok_spec, tok_spec, w_spec, w_spec, w_spec, tok_spec), out_specs=(tok_spec, tok_spec, w_spec, w_spec, w_spec), check_vma=False)
```

```python
import functools

import jax
import jax.numpy as jnp
from jax import lax
from jax.experimental import pallas as pl
from jax.experimental.pallas import tpu as pltpu
from jax.sharding import PartitionSpec as P


F32 = jnp.float32
BF16 = jnp.bfloat16
LIST = 264
GROUP = 8
PER_SRC = 256
TILE = 256
TILE_GROUPS = TILE // GROUP
LANES = 128
SUB = 4
STAGE_ROWS = 128
STAGE_SLOTS = 8
VMEM_LIMIT = 66 * 1000 * 1000


def dot_nn(a, b):
    return lax.dot_general(a, b, (((1,), (0,)), ((), ())), preferred_element_type=F32)


def dot_nt(a, b):
    return lax.dot_general(a, b, (((1,), (1,)), ((), ())), preferred_element_type=F32)


def dot_tn(a, b):
    return lax.dot_general(a, b, (((0,), (0,)), ((), ())), preferred_element_type=F32)


def route_kernel(n_tok, top_k, n_local, n_dev, dummy, idx_ref, val_ref, out_ref, ptr_ref):
    per_pair = val_ref.shape[0] > 1

    @pl.loop(0, n_local * n_dev)
    def _(e):
        ptr_ref[e] = e * LIST

    @pl.loop(0, n_tok)
    def _(t):
        token = None if per_pair else (val_ref[0] + t) * SUB
        half = top_k // 2
        for part in range(2):
            at = t * top_k + part * half
            experts = [idx_ref[at + j] for j in range(half)]
            ptrs = [ptr_ref[e] for e in experts]
            vals = [val_ref[at + j] if per_pair else token for j in range(half)]
            for e, p, v in zip(experts, ptrs, vals):
                out_ref[p] = v
                ptr_ref[e] = p + 1

    @pl.loop(0, n_local * n_dev)
    def _(e):
        p = ptr_ref[e]
        for k in range(GROUP - 1):
            out_ref[p + k] = dummy
        out_ref[e * LIST + LIST - 1] = (p - e * LIST).astype(out_ref.dtype)


def route_lists(idx, vals, n_tok, n_local, n_dev, dummy):
    n_pair = idx.shape[0]
    smem = pl.BlockSpec(memory_space=pltpu.SMEM)
    return pl.pallas_call(
        functools.partial(route_kernel, n_tok, n_pair // n_tok, n_local, n_dev, dummy),
        out_shape=jax.ShapeDtypeStruct((n_dev * n_local * LIST,), vals.dtype),
        in_specs=[smem, smem],
        out_specs=smem,
        scratch_shapes=[pltpu.SMEM((n_local * n_dev,), jnp.int32)],
        cost_estimate=pl.CostEstimate(flops=40 * 10**8, bytes_accessed=8 * n_local * n_dev * LIST, transcendentals=0),
        name='route_lists',
    )(idx, vals)


def load_table(src_hbm, table, stage, sem, n_rows, n_col):
    n_chunk = n_rows // STAGE_ROWS

    def fetch(i):
        slot = lax.rem(i, STAGE_SLOTS)
        return pltpu.make_async_copy(src_hbm.at[pl.ds(pl.multiple_of(i * STAGE_ROWS, STAGE_ROWS), STAGE_ROWS)], stage.at[slot], sem.at[slot])

    for k in range(min(STAGE_SLOTS, n_chunk)):
        fetch(jnp.int32(k)).start()

    @pl.loop(0, n_chunk)
    def _(i):
        fetch(i).wait()
        rows = stage[lax.rem(i, STAGE_SLOTS)]
        for c in range(n_col):
            table[pl.ds(i * (STAGE_ROWS * n_col) + c, STAGE_ROWS, stride=n_col), :] = rows[:, c * LANES:(c + 1) * LANES].astype(F32)

        @pl.when(i + STAGE_SLOTS < n_chunk)
        def _():
            fetch(i + STAGE_SLOTS).start()

    table[pl.ds(n_rows * n_col, 8), :] = jnp.zeros((8, LANES), F32)


SLOT = 4 * (PER_SRC // GROUP) + TILE_GROUPS + 16


def rows_at(first, n_col):
    return pl.ds(pl.multiple_of(first, n_col), n_col)


def n_groups(tok, p, e, n_local):
    return lax.div(tok[(p * n_local + e) * LIST + LIST - 1] + (GROUP - 1), GROUP)


def n_tiles(tok, e, n_src, n_local):
    groups = n_groups(tok, 0, e, n_local)
    for p in range(1, n_src):
        groups = groups + n_groups(tok, p, e, n_local)
    return lax.div(groups + (TILE_GROUPS - 1), TILE_GROUPS)


def list_groups(tok, grp, e, n_src, n_local):
    empty = n_src * n_local * LIST
    at = lax.rem(e, 3) * SLOT
    for p in range(n_src):
        base = (p * n_local + e) * LIST
        groups = n_groups(tok, p, e, n_local)

        @pl.loop(0, lax.div(groups + 3, 4))
        def _(i, base=base, at=at):
            for k in range(4):
                grp[at + 4 * i + k] = base + (4 * i + k) * GROUP

        at = at + groups
    for k in range(TILE_GROUPS):
        grp[at + k] = empty


def start_groups(tok, grp, n_src, n_local):
    for k in range(TILE_GROUPS):
        grp[3 * SLOT + k] = n_src * n_local * LIST
    list_groups(tok, grp, jnp.int32(0), n_src, n_local)


def pick_group(tok, g, tables, bufs, base, row, n_col):
    for k in range(GROUP):
        src = rows_at(tok[base + k], n_col)
        dst = pl.ds(row * n_col + k * n_col, n_col)
        bufs[0][dst, :] = tables[0][src, :]
        if len(tables) > 1:
            bufs[1][dst, :] = tables[1][src, :] * g[base + k]


def add_groups(tok, g, acc, buf, bases, row, n_col):
    dsts, rows = [], []
    for q, base in enumerate(bases):
        for k in range(GROUP):
            dsts.append(rows_at(tok[base + k], n_col))
            val = buf[pl.ds((row + q * GROUP + k) * n_col, n_col), :]
            rows.append(val if g is None else val * g[base + k])
    sums = [acc[d, :] + r for d, r in zip(dsts, rows)]
    for d, r in zip(dsts, sums):
        acc[d, :] = r


def tile_rows(buf, n_col):
    return jnp.concatenate([buf[pl.ds(c, TILE, stride=n_col), :] for c in range(n_col)], axis=1).astype(BF16)


def put_rows(buf, rows, n_col):
    for c in range(n_col):
        buf[pl.ds(c, TILE, stride=n_col), :] = rows[:, c * LANES:(c + 1) * LANES].astype(F32)


def pipelined_tiles(e, n_src, n_local, n_col, tok, g, grp, prev, tables, pick_bufs, acc, out_buf, compute):
    tiles = n_tiles(tok, e, n_src, n_local)
    here = lax.rem(e, 3) * SLOT
    following = lax.rem(e + 1, 3) * SLOT

    @pl.when(e == 0)
    def _():
        prev[0] = 3 * SLOT
        start_groups(tok, grp, n_src, n_local)

        @pl.loop(0, TILE_GROUPS)
        def _(q):
            pick_group(tok, g, tables, pick_bufs, grp[q], pl.multiple_of(q * GROUP, GROUP), n_col)

    list_groups(tok, grp, lax.min(e + 1, n_local - 1), n_src, n_local)

    @pl.loop(0, tiles)
    def _(i):
        last = prev[0]
        coming = jnp.where(i + 1 < tiles, here + (i + 1) * TILE_GROUPS, following)

        def side(part, parts):
            per = TILE_GROUPS // parts
            for q in range(part * per, (part + 1) * per, 2):
                add_groups(tok, g, acc, out_buf, [grp[last + q], grp[last + q + 1]], q * GROUP, n_col)
                for r in (q, q + 1):
                    pick_group(tok, g, tables, pick_bufs, grp[coming + r], r * GROUP, n_col)

        compute(i, side)
        prev[0] = here + i * TILE_GROUPS

    @pl.when(e == n_local - 1)
    def _():
        @pl.loop(0, TILE_GROUPS)
        def _(q):
            add_groups(tok, g, acc, out_buf, [grp[prev[0] + q]], pl.multiple_of(q * GROUP, GROUP), n_col)


def forward_kernel(n_src, n_local, n_rows, n_col, tok_hbm, g_hbm, x_hbm, dy_hbm, w_one, w_three, w_two, y_hbm, d_ref, tiles_ref, x_table, d_table, acc, x_buf, d_buf, out_buf, stage, grp, prev, sem, list_sem, tok, g):
    e = pl.program_id(0)

    @pl.when(e == 0)
    def _():
        lists = [pltpu.make_async_copy(tok_hbm, tok, list_sem.at[0]), pltpu.make_async_copy(g_hbm, g, list_sem.at[1])]
        for copy in lists:
            copy.start()
        acc[...] = jnp.zeros_like(acc)
        load_table(x_hbm, x_table, stage, sem, n_rows, n_col)
        load_table(dy_hbm, d_table, stage, sem, n_rows, n_col)
        for copy in lists:
            copy.wait()

    tiles_ref[e] = n_tiles(tok, e, n_src, n_local)

    def compute(i, side):
        rows = pl.ds(pl.multiple_of(i * TILE, TILE), TILE)
        x = tile_rows(x_buf, n_col)
        d_ref[0, rows, :] = tile_rows(d_buf, n_col)
        side(0, 4)
        pre_one = dot_nn(x, w_one[0])
        side(1, 4)
        pre_three = dot_nn(x, w_three[0])
        side(2, 4)
        hidden = (pre_one * jax.nn.sigmoid(pre_one) * pre_three).astype(BF16)
        side(3, 4)
        put_rows(out_buf, dot_nn(hidden, w_two[0]).astype(BF16), n_col)

    pipelined_tiles(e, n_src, n_local, n_col, tok, g, grp, prev, (x_table, d_table), (x_buf, d_buf), acc, out_buf, compute)

    @pl.when(e == n_local - 1)
    def _():
        out = pltpu.make_async_copy(acc.at[pl.ds(0, n_rows * n_col)], y_hbm, sem.at[0])
        out.start()
        out.wait()


def kernel_scratch(n_rows, model, n_table, n_pick):
    n_col = model // LANES
    table = pltpu.VMEM((n_rows * n_col + 8, LANES), F32)
    tile = pltpu.VMEM((TILE * n_col, LANES), F32)
    return [table] * (n_table + 1) + [tile] * (n_pick + 1) + [
        pltpu.VMEM((STAGE_SLOTS, STAGE_ROWS, model), BF16),
        pltpu.SMEM((3 * SLOT + TILE_GROUPS,), jnp.int32),
        pltpu.SMEM((1,), jnp.int32),
        pltpu.SemaphoreType.DMA((STAGE_SLOTS,)),
        pltpu.SemaphoreType.DMA((2,)),
    ]


def per_expert(a, b):
    return pl.BlockSpec((1, a, b), lambda e: (e, 0, 0))


def forward_partial(tok, g, x_all, dy_all, w_one, w_three, w_two, n_src):
    n_rows, model = x_all.shape
    n_local, _, ffn = w_one.shape
    n_col = model // LANES
    cap = n_src * PER_SRC
    smem = pl.BlockSpec(memory_space=pltpu.SMEM)
    hbm = pl.BlockSpec(memory_space=pl.ANY)
    pairs = n_rows * 8 // n_src
    return pl.pallas_call(
        functools.partial(forward_kernel, n_src, n_local, n_rows, n_col),
        out_shape=(jax.ShapeDtypeStruct((n_rows * n_col, LANES), F32), jax.ShapeDtypeStruct((n_local, cap, model), BF16), jax.ShapeDtypeStruct((n_local,), jnp.int32)),
        grid=(n_local,),
        in_specs=[hbm, hbm, hbm, hbm, per_expert(model, ffn), per_expert(model, ffn), per_expert(ffn, model)],
        out_specs=(hbm, per_expert(cap, model), smem),
        scratch_shapes=kernel_scratch(n_rows, model, 2, 2) + [pltpu.SMEM(tok.shape, tok.dtype), pltpu.SMEM(g.shape, g.dtype)],
        compiler_params=pltpu.CompilerParams(dimension_semantics=('arbitrary',), vmem_limit_bytes=VMEM_LIMIT),
        cost_estimate=pl.CostEstimate(flops=6 * pairs * model * ffn, bytes_accessed=6 * n_local * model * ffn, transcendentals=0),
        name='forward_partial',
    )(tok, g, x_all, dy_all, w_one, w_three, w_two)


def backward_kernel(n_src, n_local, n_rows, n_col, n_part, tok_hbm, x_hbm, d_ref, w_one, w_three, w_two, *rest):
    parts, rest = rest[:n_part], rest[n_part:]
    x_ref, h_ref, d1_ref, d3_ref, table, acc, x_buf, out_buf, stage, grp, prev, sem, list_sem, tok = rest
    e = pl.program_id(0)

    @pl.when(e == 0)
    def _():
        lists = pltpu.make_async_copy(tok_hbm, tok, list_sem.at[0])
        lists.start()
        acc[...] = jnp.zeros_like(acc)
        load_table(x_hbm, table, stage, sem, n_rows, n_col)
        lists.wait()

    def compute(i, side):
        rows = pl.ds(pl.multiple_of(i * TILE, TILE), TILE)
        x = tile_rows(x_buf, n_col)
        x_ref[0, rows, :] = x
        side(0, 4)
        pre_one = dot_nn(x, w_one[0])
        side(1, 4)
        pre_three = dot_nn(x, w_three[0])
        side(2, 4)
        d_hidden = dot_nt(d_ref[0, rows, :], w_two[0]).astype(BF16).astype(F32)
        side(3, 4)
        sig_one = jax.nn.sigmoid(pre_one)
        act_one = pre_one * sig_one
        h_ref[0, rows, :] = (act_one * pre_three).astype(BF16)
        d_three = (d_hidden * act_one).astype(BF16)
        d_one = (d_hidden * pre_three * sig_one * (1.0 + pre_one * (1.0 - sig_one))).astype(BF16)
        d1_ref[0, rows, :] = d_one
        d3_ref[0, rows, :] = d_three
        dx = dot_nt(d_one, w_one[0]) + dot_nt(d_three, w_three[0])
        put_rows(out_buf, dx.astype(BF16), n_col)

    pipelined_tiles(e, n_src, n_local, n_col, tok, None, grp, prev, (table,), (x_buf,), acc, out_buf, compute)

    @pl.when(e == n_local - 1)
    def _():
        own = n_rows * n_col // n_src
        part = own // n_part
        outs = [
            pltpu.make_async_copy(acc.at[pl.ds(q * own + k * part, part)], parts[k].at[pl.ds(q * part, part)], sem.at[0])
            for k in range(n_part) for q in range(n_src)
        ]
        for out in outs:
            out.start()
        for out in outs:
            out.wait()


def backward_partial(tok, x_all, d_rows, w_one, w_three, w_two, n_src, n_part):
    n_rows, model = x_all.shape
    n_local, cap, _ = d_rows.shape
    ffn = w_one.shape[2]
    n_col = model // LANES
    hbm = pl.BlockSpec(memory_space=pl.ANY)
    ffn_out = jax.ShapeDtypeStruct((n_local, cap, ffn), BF16)
    pairs = n_rows * 8 // n_src
    outs = pl.pallas_call(
        functools.partial(backward_kernel, n_src, n_local, n_rows, n_col, n_part),
        out_shape=(jax.ShapeDtypeStruct((n_rows * n_col // n_part, LANES), F32),) * n_part + (jax.ShapeDtypeStruct((n_local, cap, model), BF16), ffn_out, ffn_out, ffn_out),
        grid=(n_local,),
        in_specs=[hbm, hbm, per_expert(cap, model), per_expert(model, ffn), per_expert(model, ffn), per_expert(ffn, model)],
        out_specs=(hbm,) * n_part + (per_expert(cap, model), per_expert(cap, ffn), per_expert(cap, ffn), per_expert(cap, ffn)),
        scratch_shapes=kernel_scratch(n_rows, model, 1, 1) + [pltpu.SMEM(tok.shape, tok.dtype)],
        compiler_params=pltpu.CompilerParams(dimension_semantics=('arbitrary',), vmem_limit_bytes=VMEM_LIMIT),
        cost_estimate=pl.CostEstimate(flops=10 * pairs * model * ffn, bytes_accessed=6 * n_local * cap * ffn, transcendentals=0),
        name='backward_partial',
    )(tok, x_all, d_rows, w_one, w_three, w_two)
    return outs[:n_part], outs[n_part:]


def grad_kernel(n_src, first, tiles, x_ref, d_ref, h_ref, d1_ref, d3_ref, *refs):
    g1_ref, g3_ref, g2_ref = refs[-3:]
    used = tiles[pl.program_id(0) + first]
    for n in range(1, n_src * PER_SRC // TILE + 1):
        @pl.when(used == n)
        def _(n=n):
            rows = pl.ds(0, n * TILE)
            g1_ref[0] = dot_tn(x_ref[0, rows, :], d1_ref[0, rows, :]).astype(BF16)
            g3_ref[0] = dot_tn(x_ref[0, rows, :], d3_ref[0, rows, :]).astype(BF16)
            g2_ref[0] = dot_tn(h_ref[0, rows, :], d_ref[0, rows, :]).astype(BF16)


def weight_grads(tiles, x_rows, d_rows, hidden, d_one, d_three, n_src, first, count, so_far):
    n_local, cap, model = x_rows.shape
    ffn = hidden.shape[2]
    block = lambda a, b: pl.BlockSpec((1, a, b), lambda e: (e + first, 0, 0))
    in_grad = jax.ShapeDtypeStruct((n_local, model, ffn), BF16)
    pairs = count * cap // 2
    return pl.pallas_call(
        functools.partial(grad_kernel, n_src, first),
        out_shape=(in_grad, in_grad, jax.ShapeDtypeStruct((n_local, ffn, model), BF16)),
        grid=(count,),
        in_specs=[pl.BlockSpec(memory_space=pltpu.SMEM), block(cap, model), block(cap, model), block(cap, ffn), block(cap, ffn), block(cap, ffn)] + [pl.BlockSpec(memory_space=pl.ANY)] * len(so_far),
        out_specs=(block(model, ffn), block(model, ffn), block(ffn, model)),
        input_output_aliases={6 + k: k for k in range(len(so_far))},
        compiler_params=pltpu.CompilerParams(dimension_semantics=('arbitrary',), vmem_limit_bytes=VMEM_LIMIT),
        cost_estimate=pl.CostEstimate(flops=6 * pairs * model * ffn, bytes_accessed=6 * count * cap * ffn, transcendentals=0),
        name='weight_grads',
    )(tiles, x_rows, d_rows, hidden, d_one, d_three, *so_far)


def solution(mesh):
    n_stage = mesh.shape['stage']
    n_dev = mesh.shape['expert']
    to_next = [(stage_idx, (stage_idx + 1) % n_stage) for stage_idx in range(n_stage)]
    to_prev = [((stage_idx + 1) % n_stage, stage_idx) for stage_idx in range(n_stage)]
    tok_spec = P('stage', 'expert', None)
    w_spec = P('stage', 'expert', None, None)

    def moe_body(x_act, route_idx, route_wts, w_one, w_three, w_two, dy_act):
        n_tok, model_dim = x_act.shape[1:]
        n_local = w_one.shape[1]
        n_rows = n_tok * n_dev
        n_col = model_dim // LANES
        w_in_one, w_in_three, w_out = w_one[0], w_three[0], w_two[0]

        def gather_tokens(rows):
            return lax.all_gather(rows, 'expert', axis=0, tiled=True)

        def scatter_sums(partial):
            own = lax.psum_scatter(partial, 'expert', scatter_dimension=0, tiled=True)
            return own.reshape(-1, model_dim).astype(BF16)

        n_list = n_local * LIST

        def to_experts(lists, dummy):
            lists = lax.all_to_all(lists.reshape(n_dev, n_list), 'expert', 0, 0, tiled=True)
            return jnp.concatenate([lists.reshape(n_dev * n_list), jnp.full((LANES,), dummy, lists.dtype)])

        idx_dst = lax.ppermute(route_idx[0], 'stage', to_next)
        wts_dst = lax.ppermute(route_wts[0], 'stage', to_next)
        x_dst = lax.ppermute(x_act[0], 'stage', to_next)
        dy_all = gather_tokens(dy_act[0])
        idx_dst = idx_dst.reshape(-1)
        wts_dst = wts_dst.reshape(-1)
        first_row = (lax.axis_index('expert') * n_tok).reshape(1)
        tok = route_lists(idx_dst, first_row, n_tok, n_local, n_dev, n_rows * n_col)
        x_dst, tok, idx_dst, wts_dst, x_again = lax.optimization_barrier((x_dst, tok, idx_dst, wts_dst, x_act[0]))
        x_all = gather_tokens(x_dst)
        x_dst_again = lax.ppermute(x_again, 'stage', to_next)
        g = route_lists(idx_dst, wts_dst, n_tok, n_local, n_dev, 0.0)
        tok, g = to_experts(tok, n_rows * n_col), to_experts(g, 0.0)
        tok, g, x_dst_again, dy_all, x_all = lax.optimization_barrier((tok, g, x_dst_again, dy_all, x_all))
        x_all_again = gather_tokens(x_dst_again)

        y_sum, d_rows, tiles = forward_partial(tok, g, x_all, dy_all, w_in_one, w_in_three, w_out, n_dev)
        y_sum, x_all_again, d_rows = lax.optimization_barrier((y_sum, x_all_again, d_rows))
        y_dst = scatter_sums(y_sum)

        (dx_low, dx_high), (x_rows, hidden, d_one, d_three) = backward_partial(tok, x_all_again, d_rows, w_in_one, w_in_three, w_out, n_dev, 2)
        dx_low = scatter_sums(dx_low)
        dx_high = scatter_sums(dx_high)
        dx_low = lax.ppermute(dx_low, 'stage', to_prev)
        dx_high = lax.ppermute(dx_high, 'stage', to_prev)
        early = n_local * 5 // 8
        grads = weight_grads(tiles, x_rows, d_rows, hidden, d_one, d_three, n_dev, 0, early, ())
        g_one, g_three, g_two = weight_grads(tiles, x_rows, d_rows, hidden, d_one, d_three, n_dev, early, n_local - early, grads)
        dx_src = jnp.concatenate([dx_low, dx_high])
        return y_dst[None], dx_src[None], g_one[None], g_three[None], g_two[None]

    return jax.shard_map(moe_body, mesh=mesh, in_specs=(tok_spec, tok_spec, tok_spec, w_spec, w_spec, w_spec, tok_spec), out_specs=(tok_spec, tok_spec, w_spec, w_spec, w_spec), check_vma=False)
```

```python
import functools

import jax
import jax.numpy as jnp
from jax import lax
from jax.experimental import pallas as pl
from jax.experimental.pallas import tpu as pltpu
from jax.sharding import PartitionSpec as P


F32 = jnp.float32
BF16 = jnp.bfloat16
LIST = 264
GROUP = 8
PER_SRC = 256
TILE = 256
TILE_GROUPS = TILE // GROUP
LANES = 128
SUB = 4
FFN_STEP = 256
STAGE_ROWS = 128
STAGE_SLOTS = 8
VMEM_LIMIT = 66 * 1000 * 1000


def dot_nn(a, b):
    return lax.dot_general(a, b, (((1,), (0,)), ((), ())), preferred_element_type=F32)


def dot_nt(a, b):
    return lax.dot_general(a, b, (((1,), (1,)), ((), ())), preferred_element_type=F32)


def dot_tn(a, b):
    return lax.dot_general(a, b, (((0,), (0,)), ((), ())), preferred_element_type=F32)


def route_kernel(n_tok, top_k, n_local, n_dev, dummy, idx_ref, val_ref, out_ref, ptr_ref):
    per_pair = val_ref.shape[0] > 1

    @pl.loop(0, n_local * n_dev)
    def _(e):
        ptr_ref[e] = e * LIST

    @pl.loop(0, n_tok)
    def _(t):
        token = None if per_pair else (val_ref[0] + t) * SUB
        half = top_k // 2
        for part in range(2):
            at = t * top_k + part * half
            experts = [idx_ref[at + j] for j in range(half)]
            ptrs = [ptr_ref[e] for e in experts]
            vals = [val_ref[at + j] if per_pair else token for j in range(half)]
            for e, p, v in zip(experts, ptrs, vals):
                out_ref[p] = v
                ptr_ref[e] = p + 1

    @pl.loop(0, n_local * n_dev)
    def _(e):
        p = ptr_ref[e]
        for k in range(GROUP - 1):
            out_ref[p + k] = dummy
        out_ref[e * LIST + LIST - 1] = (p - e * LIST).astype(out_ref.dtype)


def route_lists(idx, vals, n_tok, n_local, n_dev, dummy):
    n_pair = idx.shape[0]
    smem = pl.BlockSpec(memory_space=pltpu.SMEM)
    return pl.pallas_call(
        functools.partial(route_kernel, n_tok, n_pair // n_tok, n_local, n_dev, dummy),
        out_shape=jax.ShapeDtypeStruct((n_dev * n_local * LIST,), vals.dtype),
        in_specs=[smem, smem],
        out_specs=smem,
        scratch_shapes=[pltpu.SMEM((n_local * n_dev,), jnp.int32)],
        cost_estimate=pl.CostEstimate(flops=40 * 10**8, bytes_accessed=8 * n_local * n_dev * LIST, transcendentals=0),
        name='route_lists',
    )(idx, vals)


def load_table(src_hbm, table, stage, sem, n_rows, n_col):
    n_chunk = n_rows // STAGE_ROWS

    def fetch(i):
        slot = lax.rem(i, STAGE_SLOTS)
        return pltpu.make_async_copy(src_hbm.at[pl.ds(pl.multiple_of(i * STAGE_ROWS, STAGE_ROWS), STAGE_ROWS)], stage.at[slot], sem.at[slot])

    for k in range(min(STAGE_SLOTS, n_chunk)):
        fetch(jnp.int32(k)).start()

    @pl.loop(0, n_chunk)
    def _(i):
        fetch(i).wait()
        rows = stage[lax.rem(i, STAGE_SLOTS)]
        for c in range(n_col):
            table[pl.ds(i * (STAGE_ROWS * n_col) + c, STAGE_ROWS, stride=n_col), :] = rows[:, c * LANES:(c + 1) * LANES].astype(F32)

        @pl.when(i + STAGE_SLOTS < n_chunk)
        def _():
            fetch(i + STAGE_SLOTS).start()

    table[pl.ds(n_rows * n_col, 8), :] = jnp.zeros((8, LANES), F32)


SLOT = 4 * (PER_SRC // GROUP) + TILE_GROUPS + 16


def rows_at(first, n_col):
    return pl.ds(pl.multiple_of(first, n_col), n_col)


def n_groups(tok, p, e, n_local):
    return lax.div(tok[(p * n_local + e) * LIST + LIST - 1] + (GROUP - 1), GROUP)


def n_tiles(tok, e, n_src, n_local):
    groups = n_groups(tok, 0, e, n_local)
    for p in range(1, n_src):
        groups = groups + n_groups(tok, p, e, n_local)
    return lax.div(groups + (TILE_GROUPS - 1), TILE_GROUPS)


def list_groups(tok, grp, e, n_src, n_local):
    empty = n_src * n_local * LIST
    at = lax.rem(e, 3) * SLOT
    for p in range(n_src):
        base = (p * n_local + e) * LIST
        groups = n_groups(tok, p, e, n_local)

        @pl.loop(0, lax.div(groups + 3, 4))
        def _(i, base=base, at=at):
            for k in range(4):
                grp[at + 4 * i + k] = base + (4 * i + k) * GROUP

        at = at + groups
    for k in range(TILE_GROUPS):
        grp[at + k] = empty


def start_groups(tok, grp, n_src, n_local):
    for k in range(TILE_GROUPS):
        grp[3 * SLOT + k] = n_src * n_local * LIST
    list_groups(tok, grp, jnp.int32(0), n_src, n_local)


def pick_group(tok, g, tables, bufs, base, row, n_col):
    for k in range(GROUP):
        src = rows_at(tok[base + k], n_col)
        dst = pl.ds(row * n_col + k * n_col, n_col)
        bufs[0][dst, :] = tables[0][src, :]
        if len(tables) > 1:
            bufs[1][dst, :] = tables[1][src, :] * g[base + k]


def add_groups(tok, g, acc, buf, bases, row, n_col):
    dsts, rows = [], []
    for q, base in enumerate(bases):
        for k in range(GROUP):
            dsts.append(rows_at(tok[base + k], n_col))
            val = buf[pl.ds((row + q * GROUP + k) * n_col, n_col), :]
            rows.append(val if g is None else val * g[base + k])
    sums = [acc[d, :] + r for d, r in zip(dsts, rows)]
    for d, r in zip(dsts, sums):
        acc[d, :] = r


def tile_rows(buf, n_col):
    return jnp.concatenate([buf[pl.ds(c, TILE, stride=n_col), :] for c in range(n_col)], axis=1).astype(BF16)


def put_rows(buf, rows, n_col):
    for c in range(n_col):
        buf[pl.ds(c, TILE, stride=n_col), :] = rows[:, c * LANES:(c + 1) * LANES].astype(F32)


def pipelined_tiles(e, n_src, n_local, n_col, tok, g, grp, prev, tables, pick_bufs, acc, out_buf, compute):
    tiles = n_tiles(tok, e, n_src, n_local)
    here = lax.rem(e, 3) * SLOT
    following = lax.rem(e + 1, 3) * SLOT

    @pl.when(e == 0)
    def _():
        prev[0] = 3 * SLOT
        start_groups(tok, grp, n_src, n_local)

        @pl.loop(0, TILE_GROUPS)
        def _(q):
            pick_group(tok, g, tables, pick_bufs, grp[q], pl.multiple_of(q * GROUP, GROUP), n_col)

    list_groups(tok, grp, lax.min(e + 1, n_local - 1), n_src, n_local)

    @pl.loop(0, tiles)
    def _(i):
        last = prev[0]
        coming = jnp.where(i + 1 < tiles, here + (i + 1) * TILE_GROUPS, following)

        def side(part, parts):
            pairs = TILE_GROUPS // 2
            for q in range(2 * (part * pairs // parts), 2 * ((part + 1) * pairs // parts), 2):
                add_groups(tok, g, acc, out_buf, [grp[last + q], grp[last + q + 1]], q * GROUP, n_col)
                for r in (q, q + 1):
                    pick_group(tok, g, tables, pick_bufs, grp[coming + r], r * GROUP, n_col)

        compute(i, side)
        prev[0] = here + i * TILE_GROUPS

    @pl.when(e == n_local - 1)
    def _():
        @pl.loop(0, TILE_GROUPS)
        def _(q):
            add_groups(tok, g, acc, out_buf, [grp[prev[0] + q]], pl.multiple_of(q * GROUP, GROUP), n_col)


def forward_kernel(n_src, n_local, n_rows, n_col, tok_hbm, g_hbm, x_hbm, dy_hbm, w_one, w_three, w_two, y_hbm, d_ref, tiles_ref, x_table, d_table, acc, x_buf, d_buf, out_buf, stage, grp, prev, sem, list_sem, tok, g):
    e = pl.program_id(0)

    @pl.when(e == 0)
    def _():
        lists = [pltpu.make_async_copy(tok_hbm, tok, list_sem.at[0]), pltpu.make_async_copy(g_hbm, g, list_sem.at[1])]
        for copy in lists:
            copy.start()
        acc[...] = jnp.zeros_like(acc)
        load_table(x_hbm, x_table, stage, sem, n_rows, n_col)
        load_table(dy_hbm, d_table, stage, sem, n_rows, n_col)
        for copy in lists:
            copy.wait()

    tiles_ref[e] = n_tiles(tok, e, n_src, n_local)

    def compute(i, side):
        rows = pl.ds(pl.multiple_of(i * TILE, TILE), TILE)
        x = tile_rows(x_buf, n_col)
        d_ref[0, rows, :] = tile_rows(d_buf, n_col)
        ffn = w_one.shape[2]
        hidden = []
        for k, f in enumerate(range(0, ffn, FFN_STEP)):
            side(k, ffn // FFN_STEP + 0)
            pre_one = dot_nn(x, w_one[0, :, f:f + FFN_STEP])
            pre_three = dot_nn(x, w_three[0, :, f:f + FFN_STEP])
            hidden.append((pre_one * jax.nn.sigmoid(pre_one) * pre_three).astype(BF16))
        put_rows(out_buf, dot_nn(jnp.concatenate(hidden, axis=1), w_two[0]).astype(BF16), n_col)

    pipelined_tiles(e, n_src, n_local, n_col, tok, g, grp, prev, (x_table, d_table), (x_buf, d_buf), acc, out_buf, compute)

    @pl.when(e == n_local - 1)
    def _():
        out = pltpu.make_async_copy(acc.at[pl.ds(0, n_rows * n_col)], y_hbm, sem.at[0])
        out.start()
        out.wait()


def kernel_scratch(n_rows, model, n_table, n_pick):
    n_col = model // LANES
    table = pltpu.VMEM((n_rows * n_col + 8, LANES), F32)
    tile = pltpu.VMEM((TILE * n_col, LANES), F32)
    return [table] * (n_table + 1) + [tile] * (n_pick + 1) + [
        pltpu.VMEM((STAGE_SLOTS, STAGE_ROWS, model), BF16),
        pltpu.SMEM((3 * SLOT + TILE_GROUPS,), jnp.int32),
        pltpu.SMEM((1,), jnp.int32),
        pltpu.SemaphoreType.DMA((STAGE_SLOTS,)),
        pltpu.SemaphoreType.DMA((2,)),
    ]


def per_expert(a, b):
    return pl.BlockSpec((1, a, b), lambda e: (e, 0, 0))


def forward_partial(tok, g, x_all, dy_all, w_one, w_three, w_two, n_src):
    n_rows, model = x_all.shape
    n_local, _, ffn = w_one.shape
    n_col = model // LANES
    cap = n_src * PER_SRC
    smem = pl.BlockSpec(memory_space=pltpu.SMEM)
    hbm = pl.BlockSpec(memory_space=pl.ANY)
    pairs = n_rows * 8 // n_src
    return pl.pallas_call(
        functools.partial(forward_kernel, n_src, n_local, n_rows, n_col),
        out_shape=(jax.ShapeDtypeStruct((n_rows * n_col, LANES), F32), jax.ShapeDtypeStruct((n_local, cap, model), BF16), jax.ShapeDtypeStruct((n_local,), jnp.int32)),
        grid=(n_local,),
        in_specs=[hbm, hbm, hbm, hbm, per_expert(model, ffn), per_expert(model, ffn), per_expert(ffn, model)],
        out_specs=(hbm, per_expert(cap, model), smem),
        scratch_shapes=kernel_scratch(n_rows, model, 2, 2) + [pltpu.SMEM(tok.shape, tok.dtype), pltpu.SMEM(g.shape, g.dtype)],
        compiler_params=pltpu.CompilerParams(dimension_semantics=('arbitrary',), vmem_limit_bytes=VMEM_LIMIT),
        cost_estimate=pl.CostEstimate(flops=6 * pairs * model * ffn, bytes_accessed=6 * n_local * model * ffn, transcendentals=0),
        name='forward_partial',
    )(tok, g, x_all, dy_all, w_one, w_three, w_two)


def backward_kernel(n_src, n_local, n_rows, n_col, n_part, tok_hbm, x_hbm, d_ref, w_one, w_three, w_two, *rest):
    parts, rest = rest[:n_part], rest[n_part:]
    x_ref, h_ref, d1_ref, d3_ref, table, acc, x_buf, out_buf, stage, grp, prev, sem, list_sem, tok = rest
    e = pl.program_id(0)

    @pl.when(e == 0)
    def _():
        lists = pltpu.make_async_copy(tok_hbm, tok, list_sem.at[0])
        lists.start()
        acc[...] = jnp.zeros_like(acc)
        load_table(x_hbm, table, stage, sem, n_rows, n_col)
        lists.wait()

    def compute(i, side):
        rows = pl.ds(pl.multiple_of(i * TILE, TILE), TILE)
        x = tile_rows(x_buf, n_col)
        x_ref[0, rows, :] = x
        d = d_ref[0, rows, :]
        ffn = w_one.shape[2]
        for k, f in enumerate(range(0, ffn, FFN_STEP)):
            cols = slice(f, f + FFN_STEP)
            side(k, ffn // FFN_STEP + 0)
            pre_one = dot_nn(x, w_one[0, :, cols])
            pre_three = dot_nn(x, w_three[0, :, cols])
            d_hidden = dot_nt(d, w_two[0, cols, :]).astype(BF16).astype(F32)
            sig_one = jax.nn.sigmoid(pre_one)
            act_one = pre_one * sig_one
            h_ref[0, rows, cols] = (act_one * pre_three).astype(BF16)
            d3_ref[0, rows, cols] = (d_hidden * act_one).astype(BF16)
            d1_ref[0, rows, cols] = (d_hidden * pre_three * sig_one * (1.0 + pre_one * (1.0 - sig_one))).astype(BF16)
        dx = dot_nt(d1_ref[0, rows, :], w_one[0]) + dot_nt(d3_ref[0, rows, :], w_three[0])
        put_rows(out_buf, dx.astype(BF16), n_col)

    pipelined_tiles(e, n_src, n_local, n_col, tok, None, grp, prev, (table,), (x_buf,), acc, out_buf, compute)

    @pl.when(e == n_local - 1)
    def _():
        own = n_rows * n_col // n_src
        part = own // n_part
        outs = [
            pltpu.make_async_copy(acc.at[pl.ds(q * own + k * part, part)], parts[k].at[pl.ds(q * part, part)], sem.at[0])
            for k in range(n_part) for q in range(n_src)
        ]
        for out in outs:
            out.start()
        for out in outs:
            out.wait()


def backward_partial(tok, x_all, d_rows, w_one, w_three, w_two, n_src, n_part):
    n_rows, model = x_all.shape
    n_local, cap, _ = d_rows.shape
    ffn = w_one.shape[2]
    n_col = model // LANES
    hbm = pl.BlockSpec(memory_space=pl.ANY)
    ffn_out = jax.ShapeDtypeStruct((n_local, cap, ffn), BF16)
    pairs = n_rows * 8 // n_src
    outs = pl.pallas_call(
        functools.partial(backward_kernel, n_src, n_local, n_rows, n_col, n_part),
        out_shape=(jax.ShapeDtypeStruct((n_rows * n_col // n_part, LANES), F32),) * n_part + (jax.ShapeDtypeStruct((n_local, cap, model), BF16), ffn_out, ffn_out, ffn_out),
        grid=(n_local,),
        in_specs=[hbm, hbm, per_expert(cap, model), per_expert(model, ffn), per_expert(model, ffn), per_expert(ffn, model)],
        out_specs=(hbm,) * n_part + (per_expert(cap, model), per_expert(cap, ffn), per_expert(cap, ffn), per_expert(cap, ffn)),
        scratch_shapes=kernel_scratch(n_rows, model, 1, 1) + [pltpu.SMEM(tok.shape, tok.dtype)],
        compiler_params=pltpu.CompilerParams(dimension_semantics=('arbitrary',), vmem_limit_bytes=VMEM_LIMIT),
        cost_estimate=pl.CostEstimate(flops=10 * pairs * model * ffn, bytes_accessed=6 * n_local * cap * ffn, transcendentals=0),
        name='backward_partial',
    )(tok, x_all, d_rows, w_one, w_three, w_two)
    return outs[:n_part], outs[n_part:]


def grad_kernel(n_src, first, tiles, x_ref, d_ref, h_ref, d1_ref, d3_ref, *refs):
    g1_ref, g3_ref, g2_ref = refs[-3:]
    used = tiles[pl.program_id(0) + first]
    for n in range(1, n_src * PER_SRC // TILE + 1):
        @pl.when(used == n)
        def _(n=n):
            rows = pl.ds(0, n * TILE)
            g1_ref[0] = dot_tn(x_ref[0, rows, :], d1_ref[0, rows, :]).astype(BF16)
            g3_ref[0] = dot_tn(x_ref[0, rows, :], d3_ref[0, rows, :]).astype(BF16)
            g2_ref[0] = dot_tn(h_ref[0, rows, :], d_ref[0, rows, :]).astype(BF16)


def weight_grads(tiles, x_rows, d_rows, hidden, d_one, d_three, n_src, first, count, so_far):
    n_local, cap, model = x_rows.shape
    ffn = hidden.shape[2]
    block = lambda a, b: pl.BlockSpec((1, a, b), lambda e: (e + first, 0, 0))
    in_grad = jax.ShapeDtypeStruct((n_local, model, ffn), BF16)
    pairs = count * cap // 2
    return pl.pallas_call(
        functools.partial(grad_kernel, n_src, first),
        out_shape=(in_grad, in_grad, jax.ShapeDtypeStruct((n_local, ffn, model), BF16)),
        grid=(count,),
        in_specs=[pl.BlockSpec(memory_space=pltpu.SMEM), block(cap, model), block(cap, model), block(cap, ffn), block(cap, ffn), block(cap, ffn)] + [pl.BlockSpec(memory_space=pl.ANY)] * len(so_far),
        out_specs=(block(model, ffn), block(model, ffn), block(ffn, model)),
        input_output_aliases={6 + k: k for k in range(len(so_far))},
        compiler_params=pltpu.CompilerParams(dimension_semantics=('arbitrary',), vmem_limit_bytes=VMEM_LIMIT),
        cost_estimate=pl.CostEstimate(flops=6 * pairs * model * ffn, bytes_accessed=6 * count * cap * ffn, transcendentals=0),
        name='weight_grads',
    )(tiles, x_rows, d_rows, hidden, d_one, d_three, *so_far)


def solution(mesh):
    n_stage = mesh.shape['stage']
    n_dev = mesh.shape['expert']
    to_next = [(stage_idx, (stage_idx + 1) % n_stage) for stage_idx in range(n_stage)]
    to_prev = [((stage_idx + 1) % n_stage, stage_idx) for stage_idx in range(n_stage)]
    tok_spec = P('stage', 'expert', None)
    w_spec = P('stage', 'expert', None, None)

    def moe_body(x_act, route_idx, route_wts, w_one, w_three, w_two, dy_act):
        n_tok, model_dim = x_act.shape[1:]
        n_local = w_one.shape[1]
        n_rows = n_tok * n_dev
        n_col = model_dim // LANES
        w_in_one, w_in_three, w_out = w_one[0], w_three[0], w_two[0]

        def gather_tokens(rows):
            return lax.all_gather(rows, 'expert', axis=0, tiled=True)

        def scatter_sums(partial):
            own = lax.psum_scatter(partial, 'expert', scatter_dimension=0, tiled=True)
            return own.reshape(-1, model_dim).astype(BF16)

        n_list = n_local * LIST

        def to_experts(lists, dummy):
            lists = lax.all_to_all(lists.reshape(n_dev, n_list), 'expert', 0, 0, tiled=True)
            return jnp.concatenate([lists.reshape(n_dev * n_list), jnp.full((LANES,), dummy, lists.dtype)])

        idx_dst = lax.ppermute(route_idx[0], 'stage', to_next)
        wts_dst = lax.ppermute(route_wts[0], 'stage', to_next)
        idx_dst, wts_dst, x_src = lax.optimization_barrier((idx_dst, wts_dst, x_act[0]))
        x_dst = lax.ppermute(x_src, 'stage', to_next)
        dy_all = gather_tokens(dy_act[0])
        idx_dst = idx_dst.reshape(-1)
        wts_dst = wts_dst.reshape(-1)
        first_row = (lax.axis_index('expert') * n_tok).reshape(1)
        tok = route_lists(idx_dst, first_row, n_tok, n_local, n_dev, n_rows * n_col)
        x_dst, tok, idx_dst, wts_dst, x_again = lax.optimization_barrier((x_dst, tok, idx_dst, wts_dst, x_act[0]))
        x_all = gather_tokens(x_dst)
        x_dst_again = lax.ppermute(x_again, 'stage', to_next)
        g = route_lists(idx_dst, wts_dst, n_tok, n_local, n_dev, 0.0)
        tok, g = to_experts(tok, n_rows * n_col), to_experts(g, 0.0)
        tok, g, x_dst_again, dy_all, x_all = lax.optimization_barrier((tok, g, x_dst_again, dy_all, x_all))
        x_all_again = gather_tokens(x_dst_again)

        y_sum, d_rows, tiles = forward_partial(tok, g, x_all, dy_all, w_in_one, w_in_three, w_out, n_dev)
        y_sum, x_all_again, d_rows = lax.optimization_barrier((y_sum, x_all_again, d_rows))
        y_dst = scatter_sums(y_sum)

        (dx_low, dx_high), (x_rows, hidden, d_one, d_three) = backward_partial(tok, x_all_again, d_rows, w_in_one, w_in_three, w_out, n_dev, 2)
        dx_low = scatter_sums(dx_low)
        dx_high = scatter_sums(dx_high)
        dx_low = lax.ppermute(dx_low, 'stage', to_prev)
        dx_high = lax.ppermute(dx_high, 'stage', to_prev)
        early = n_local * 5 // 8
        grads = weight_grads(tiles, x_rows, d_rows, hidden, d_one, d_three, n_dev, 0, early, ())
        g_one, g_three, g_two = weight_grads(tiles, x_rows, d_rows, hidden, d_one, d_three, n_dev, early, n_local - early, grads)
        dx_src = jnp.concatenate([dx_low, dx_high])
        return y_dst[None], dx_src[None], g_one[None], g_three[None], g_two[None]

    return jax.shard_map(moe_body, mesh=mesh, in_specs=(tok_spec, tok_spec, tok_spec, w_spec, w_spec, w_spec, tok_spec), out_specs=(tok_spec, tok_spec, w_spec, w_spec, w_spec), check_vma=False)
```

```python
import functools

import jax
import jax.numpy as jnp
from jax import lax
from jax.experimental import pallas as pl
from jax.experimental.pallas import tpu as pltpu
from jax.sharding import PartitionSpec as P


F32 = jnp.float32
BF16 = jnp.bfloat16
LIST = 264
GROUP = 8
PER_SRC = 256
TILE = 256
TILE_GROUPS = TILE // GROUP
LANES = 128
SUB = 4
FFN_STEP = 256
STAGE_ROWS = 128
STAGE_SLOTS = 8
VMEM_LIMIT = 66 * 1000 * 1000


def dot_nn(a, b):
    return lax.dot_general(a, b, (((1,), (0,)), ((), ())), preferred_element_type=F32)


def dot_nt(a, b):
    return lax.dot_general(a, b, (((1,), (1,)), ((), ())), preferred_element_type=F32)


def dot_tn(a, b):
    return lax.dot_general(a, b, (((0,), (0,)), ((), ())), preferred_element_type=F32)


def route_kernel(n_tok, top_k, n_local, n_dev, dummy, idx_ref, val_ref, out_ref, ptr_ref):
    per_pair = val_ref.shape[0] > 1

    @pl.loop(0, n_local * n_dev)
    def _(e):
        ptr_ref[e] = e * LIST

    @pl.loop(0, n_tok)
    def _(t):
        token = None if per_pair else (val_ref[0] + t) * SUB
        half = top_k // 2
        for part in range(2):
            at = t * top_k + part * half
            experts = [idx_ref[at + j] for j in range(half)]
            ptrs = [ptr_ref[e] for e in experts]
            vals = [val_ref[at + j] if per_pair else token for j in range(half)]
            for e, p, v in zip(experts, ptrs, vals):
                out_ref[p] = v
                ptr_ref[e] = p + 1

    @pl.loop(0, n_local * n_dev)
    def _(e):
        p = ptr_ref[e]
        for k in range(GROUP - 1):
            out_ref[p + k] = dummy
        out_ref[e * LIST + LIST - 1] = (p - e * LIST).astype(out_ref.dtype)


def route_lists(idx, vals, n_tok, n_local, n_dev, dummy):
    n_pair = idx.shape[0]
    smem = pl.BlockSpec(memory_space=pltpu.SMEM)
    return pl.pallas_call(
        functools.partial(route_kernel, n_tok, n_pair // n_tok, n_local, n_dev, dummy),
        out_shape=jax.ShapeDtypeStruct((n_dev * n_local * LIST,), vals.dtype),
        in_specs=[smem, smem],
        out_specs=smem,
        scratch_shapes=[pltpu.SMEM((n_local * n_dev,), jnp.int32)],
        cost_estimate=pl.CostEstimate(flops=40 * 10**8, bytes_accessed=8 * n_local * n_dev * LIST, transcendentals=0),
        name='route_lists',
    )(idx, vals)


def load_table(src_hbm, table, stage, sem, n_rows, n_col):
    n_chunk = n_rows // STAGE_ROWS

    def fetch(i):
        slot = lax.rem(i, STAGE_SLOTS)
        return pltpu.make_async_copy(src_hbm.at[pl.ds(pl.multiple_of(i * STAGE_ROWS, STAGE_ROWS), STAGE_ROWS)], stage.at[slot], sem.at[slot])

    for k in range(min(STAGE_SLOTS, n_chunk)):
        fetch(jnp.int32(k)).start()

    @pl.loop(0, n_chunk)
    def _(i):
        fetch(i).wait()
        rows = stage[lax.rem(i, STAGE_SLOTS)]
        for c in range(n_col):
            table[pl.ds(i * (STAGE_ROWS * n_col) + c, STAGE_ROWS, stride=n_col), :] = rows[:, c * LANES:(c + 1) * LANES].astype(F32)

        @pl.when(i + STAGE_SLOTS < n_chunk)
        def _():
            fetch(i + STAGE_SLOTS).start()

    table[pl.ds(n_rows * n_col, 8), :] = jnp.zeros((8, LANES), F32)


SLOT = 4 * (PER_SRC // GROUP) + TILE_GROUPS + 16


def rows_at(first, n_col):
    return pl.ds(pl.multiple_of(first, n_col), n_col)


def n_groups(tok, p, e, n_local):
    return lax.div(tok[(p * n_local + e) * LIST + LIST - 1] + (GROUP - 1), GROUP)


def n_tiles(tok, e, n_src, n_local):
    groups = n_groups(tok, 0, e, n_local)
    for p in range(1, n_src):
        groups = groups + n_groups(tok, p, e, n_local)
    return lax.div(groups + (TILE_GROUPS - 1), TILE_GROUPS)


def list_groups(tok, grp, e, n_src, n_local):
    empty = n_src * n_local * LIST
    at = lax.rem(e, 3) * SLOT
    for p in range(n_src):
        base = (p * n_local + e) * LIST
        groups = n_groups(tok, p, e, n_local)

        @pl.loop(0, lax.div(groups + 3, 4))
        def _(i, base=base, at=at):
            for k in range(4):
                grp[at + 4 * i + k] = base + (4 * i + k) * GROUP

        at = at + groups
    for k in range(TILE_GROUPS):
        grp[at + k] = empty


def start_groups(tok, grp, n_src, n_local):
    for k in range(TILE_GROUPS):
        grp[3 * SLOT + k] = n_src * n_local * LIST
    list_groups(tok, grp, jnp.int32(0), n_src, n_local)


def pick_group(tok, g, tables, bufs, base, row, n_col):
    for k in range(GROUP):
        src = rows_at(tok[base + k], n_col)
        dst = pl.ds(row * n_col + k * n_col, n_col)
        bufs[0][dst, :] = tables[0][src, :]
        if len(tables) > 1:
            bufs[1][dst, :] = tables[1][src, :] * g[base + k]


def add_group(tok, g, acc, buf, base, row, n_col, step):
    for first in range(0, GROUP, step):
        dsts, rows = [], []
        for k in range(first, first + step):
            dsts.append(rows_at(tok[base + k], n_col))
            val = buf[pl.ds((row + k) * n_col, n_col), :]
            rows.append(val if g is None else val * g[base + k])
        sums = [acc[d, :] + r for d, r in zip(dsts, rows)]
        for d, r in zip(dsts, sums):
            acc[d, :] = r


def tile_rows(buf, n_col):
    return jnp.concatenate([buf[pl.ds(c, TILE, stride=n_col), :] for c in range(n_col)], axis=1).astype(BF16)


def put_rows(buf, rows, n_col):
    for c in range(n_col):
        buf[pl.ds(c, TILE, stride=n_col), :] = rows[:, c * LANES:(c + 1) * LANES].astype(F32)


def pipelined_tiles(e, n_src, n_local, n_col, tok, g, grp, prev, tables, pick_bufs, acc, out_buf, step, compute):
    tiles = n_tiles(tok, e, n_src, n_local)
    here = lax.rem(e, 3) * SLOT
    following = lax.rem(e + 1, 3) * SLOT

    @pl.when(e == 0)
    def _():
        prev[0] = 3 * SLOT
        start_groups(tok, grp, n_src, n_local)

        @pl.loop(0, TILE_GROUPS)
        def _(q):
            pick_group(tok, g, tables, pick_bufs, grp[q], pl.multiple_of(q * GROUP, GROUP), n_col)

    list_groups(tok, grp, lax.min(e + 1, n_local - 1), n_src, n_local)

    @pl.loop(0, tiles)
    def _(i):
        last = prev[0]
        coming = jnp.where(i + 1 < tiles, here + (i + 1) * TILE_GROUPS, following)

        def side(part, parts):
            for q in range(part * TILE_GROUPS // parts, (part + 1) * TILE_GROUPS // parts):
                add_group(tok, g, acc, out_buf, grp[last + q], q * GROUP, n_col, step)
                pick_group(tok, g, tables, pick_bufs, grp[coming + q], q * GROUP, n_col)

        compute(i, side)
        prev[0] = here + i * TILE_GROUPS

    @pl.when(e == n_local - 1)
    def _():
        @pl.loop(0, TILE_GROUPS)
        def _(q):
            add_group(tok, g, acc, out_buf, grp[prev[0] + q], pl.multiple_of(q * GROUP, GROUP), n_col, step)


def forward_kernel(n_src, n_local, n_rows, n_col, tok_hbm, g_hbm, x_hbm, dy_hbm, w_one, w_three, w_two, y_hbm, d_ref, tiles_ref, x_table, d_table, acc, x_buf, d_buf, out_buf, stage, grp, prev, sem, list_sem, tok, g):
    e = pl.program_id(0)

    @pl.when(e == 0)
    def _():
        lists = [pltpu.make_async_copy(tok_hbm, tok, list_sem.at[0]), pltpu.make_async_copy(g_hbm, g, list_sem.at[1])]
        for copy in lists:
            copy.start()
        acc[...] = jnp.zeros_like(acc)
        load_table(x_hbm, x_table, stage, sem, n_rows, n_col)
        load_table(dy_hbm, d_table, stage, sem, n_rows, n_col)
        for copy in lists:
            copy.wait()

    tiles_ref[e] = n_tiles(tok, e, n_src, n_local)

    def compute(i, side):
        rows = pl.ds(pl.multiple_of(i * TILE, TILE), TILE)
        x = tile_rows(x_buf, n_col)
        d_ref[0, rows, :] = tile_rows(d_buf, n_col)
        ffn = w_one.shape[2]
        hidden = []
        for k, f in enumerate(range(0, ffn, FFN_STEP)):
            side(k, ffn // FFN_STEP)
            pre_one = dot_nn(x, w_one[0, :, f:f + FFN_STEP])
            pre_three = dot_nn(x, w_three[0, :, f:f + FFN_STEP])
            hidden.append((pre_one * jax.nn.sigmoid(pre_one) * pre_three).astype(BF16))
        put_rows(out_buf, dot_nn(jnp.concatenate(hidden, axis=1), w_two[0]).astype(BF16), n_col)

    pipelined_tiles(e, n_src, n_local, n_col, tok, g, grp, prev, (x_table, d_table), (x_buf, d_buf), acc, out_buf, GROUP, compute)

    @pl.when(e == n_local - 1)
    def _():
        out = pltpu.make_async_copy(acc.at[pl.ds(0, n_rows * n_col)], y_hbm, sem.at[0])
        out.start()
        out.wait()


def kernel_scratch(n_rows, model, n_table, n_pick):
    n_col = model // LANES
    table = pltpu.VMEM((n_rows * n_col + 8, LANES), F32)
    tile = pltpu.VMEM((TILE * n_col, LANES), F32)
    return [table] * (n_table + 1) + [tile] * (n_pick + 1) + [
        pltpu.VMEM((STAGE_SLOTS, STAGE_ROWS, model), BF16),
        pltpu.SMEM((3 * SLOT + TILE_GROUPS,), jnp.int32),
        pltpu.SMEM((1,), jnp.int32),
        pltpu.SemaphoreType.DMA((STAGE_SLOTS,)),
        pltpu.SemaphoreType.DMA((2,)),
    ]


def per_expert(a, b):
    return pl.BlockSpec((1, a, b), lambda e: (e, 0, 0))


def forward_partial(tok, g, x_all, dy_all, w_one, w_three, w_two, n_src):
    n_rows, model = x_all.shape
    n_local, _, ffn = w_one.shape
    n_col = model // LANES
    cap = n_src * PER_SRC
    smem = pl.BlockSpec(memory_space=pltpu.SMEM)
    hbm = pl.BlockSpec(memory_space=pl.ANY)
    pairs = n_rows * 8 // n_src
    return pl.pallas_call(
        functools.partial(forward_kernel, n_src, n_local, n_rows, n_col),
        out_shape=(jax.ShapeDtypeStruct((n_rows * n_col, LANES), F32), jax.ShapeDtypeStruct((n_local, cap, model), BF16), jax.ShapeDtypeStruct((n_local,), jnp.int32)),
        grid=(n_local,),
        in_specs=[hbm, hbm, hbm, hbm, per_expert(model, ffn), per_expert(model, ffn), per_expert(ffn, model)],
        out_specs=(hbm, per_expert(cap, model), smem),
        scratch_shapes=kernel_scratch(n_rows, model, 2, 2) + [pltpu.SMEM(tok.shape, tok.dtype), pltpu.SMEM(g.shape, g.dtype)],
        compiler_params=pltpu.CompilerParams(dimension_semantics=('arbitrary',), vmem_limit_bytes=VMEM_LIMIT),
        cost_estimate=pl.CostEstimate(flops=6 * pairs * model * ffn, bytes_accessed=6 * n_local * model * ffn, transcendentals=0),
        name='forward_partial',
    )(tok, g, x_all, dy_all, w_one, w_three, w_two)


def backward_kernel(n_src, n_local, n_rows, n_col, cuts, tok_hbm, x_hbm, d_ref, w_one, w_three, w_two, *rest):
    n_part = len(cuts) - 1
    parts, rest = rest[:n_part], rest[n_part:]
    x_ref, h_ref, d1_ref, d3_ref, table, acc, x_buf, out_buf, stage, grp, prev, sem, list_sem, tok = rest
    e = pl.program_id(0)

    @pl.when(e == 0)
    def _():
        lists = pltpu.make_async_copy(tok_hbm, tok, list_sem.at[0])
        lists.start()
        acc[...] = jnp.zeros_like(acc)
        load_table(x_hbm, table, stage, sem, n_rows, n_col)
        lists.wait()

    def compute(i, side):
        rows = pl.ds(pl.multiple_of(i * TILE, TILE), TILE)
        x = tile_rows(x_buf, n_col)
        x_ref[0, rows, :] = x
        d = d_ref[0, rows, :]
        ffn = w_one.shape[2]
        for k, f in enumerate(range(0, ffn, FFN_STEP)):
            cols = slice(f, f + FFN_STEP)
            side(k, ffn // FFN_STEP)
            pre_one = dot_nn(x, w_one[0, :, cols])
            pre_three = dot_nn(x, w_three[0, :, cols])
            d_hidden = dot_nt(d, w_two[0, cols, :]).astype(BF16).astype(F32)
            sig_one = jax.nn.sigmoid(pre_one)
            act_one = pre_one * sig_one
            h_ref[0, rows, cols] = (act_one * pre_three).astype(BF16)
            d3_ref[0, rows, cols] = (d_hidden * act_one).astype(BF16)
            d1_ref[0, rows, cols] = (d_hidden * pre_three * sig_one * (1.0 + pre_one * (1.0 - sig_one))).astype(BF16)
        dx = dot_nt(d1_ref[0, rows, :], w_one[0]) + dot_nt(d3_ref[0, rows, :], w_three[0])
        put_rows(out_buf, dx.astype(BF16), n_col)

    pipelined_tiles(e, n_src, n_local, n_col, tok, None, grp, prev, (table,), (x_buf,), acc, out_buf, GROUP // 2, compute)

    @pl.when(e == n_local - 1)
    def _():
        own = n_rows * n_col // n_src
        outs = []
        for k, (lo, hi) in enumerate(zip(cuts, cuts[1:])):
            part = (hi - lo) * n_col
            outs += [pltpu.make_async_copy(acc.at[pl.ds(q * own + lo * n_col, part)], parts[k].at[pl.ds(q * part, part)], sem.at[0]) for q in range(n_src)]
        for out in outs:
            out.start()
        for out in outs:
            out.wait()


def backward_partial(tok, x_all, d_rows, w_one, w_three, w_two, n_src, cuts):
    n_rows, model = x_all.shape
    n_local, cap, _ = d_rows.shape
    ffn = w_one.shape[2]
    n_col = model // LANES
    hbm = pl.BlockSpec(memory_space=pl.ANY)
    ffn_out = jax.ShapeDtypeStruct((n_local, cap, ffn), BF16)
    pairs = n_rows * 8 // n_src
    n_part = len(cuts) - 1
    outs = pl.pallas_call(
        functools.partial(backward_kernel, n_src, n_local, n_rows, n_col, cuts),
        out_shape=tuple(jax.ShapeDtypeStruct((n_src * (hi - lo) * n_col, LANES), F32) for lo, hi in zip(cuts, cuts[1:])) + (jax.ShapeDtypeStruct((n_local, cap, model), BF16), ffn_out, ffn_out, ffn_out),
        grid=(n_local,),
        in_specs=[hbm, hbm, per_expert(cap, model), per_expert(model, ffn), per_expert(model, ffn), per_expert(ffn, model)],
        out_specs=(hbm,) * n_part + (per_expert(cap, model), per_expert(cap, ffn), per_expert(cap, ffn), per_expert(cap, ffn)),
        scratch_shapes=kernel_scratch(n_rows, model, 1, 1) + [pltpu.SMEM(tok.shape, tok.dtype)],
        compiler_params=pltpu.CompilerParams(dimension_semantics=('arbitrary',), vmem_limit_bytes=VMEM_LIMIT),
        cost_estimate=pl.CostEstimate(flops=10 * pairs * model * ffn, bytes_accessed=6 * n_local * cap * ffn, transcendentals=0),
        name='backward_partial',
    )(tok, x_all, d_rows, w_one, w_three, w_two)
    return outs[:n_part], outs[n_part:]


def grad_kernel(n_src, first, tiles, x_ref, d_ref, h_ref, d1_ref, d3_ref, *refs):
    g1_ref, g3_ref, g2_ref = refs[-3:]
    used = tiles[pl.program_id(0) + first]
    for n in range(1, n_src * PER_SRC // TILE + 1):
        @pl.when(used == n)
        def _(n=n):
            rows = pl.ds(0, n * TILE)
            g1_ref[0] = dot_tn(x_ref[0, rows, :], d1_ref[0, rows, :]).astype(BF16)
            g3_ref[0] = dot_tn(x_ref[0, rows, :], d3_ref[0, rows, :]).astype(BF16)
            g2_ref[0] = dot_tn(h_ref[0, rows, :], d_ref[0, rows, :]).astype(BF16)


def weight_grads(tiles, x_rows, d_rows, hidden, d_one, d_three, n_src, first, count, so_far):
    n_local, cap, model = x_rows.shape
    ffn = hidden.shape[2]
    block = lambda a, b: pl.BlockSpec((1, a, b), lambda e: (e + first, 0, 0))
    in_grad = jax.ShapeDtypeStruct((n_local, model, ffn), BF16)
    pairs = count * cap // 2
    return pl.pallas_call(
        functools.partial(grad_kernel, n_src, first),
        out_shape=(in_grad, in_grad, jax.ShapeDtypeStruct((n_local, ffn, model), BF16)),
        grid=(count,),
        in_specs=[pl.BlockSpec(memory_space=pltpu.SMEM), block(cap, model), block(cap, model), block(cap, ffn), block(cap, ffn), block(cap, ffn)] + [pl.BlockSpec(memory_space=pl.ANY)] * len(so_far),
        out_specs=(block(model, ffn), block(model, ffn), block(ffn, model)),
        input_output_aliases={6 + k: k for k in range(len(so_far))},
        compiler_params=pltpu.CompilerParams(dimension_semantics=('arbitrary',), vmem_limit_bytes=VMEM_LIMIT),
        cost_estimate=pl.CostEstimate(flops=6 * pairs * model * ffn, bytes_accessed=6 * count * cap * ffn, transcendentals=0),
        name='weight_grads',
    )(tiles, x_rows, d_rows, hidden, d_one, d_three, *so_far)


def solution(mesh):
    n_stage = mesh.shape['stage']
    n_dev = mesh.shape['expert']
    to_next = [(stage_idx, (stage_idx + 1) % n_stage) for stage_idx in range(n_stage)]
    to_prev = [((stage_idx + 1) % n_stage, stage_idx) for stage_idx in range(n_stage)]
    tok_spec = P('stage', 'expert', None)
    w_spec = P('stage', 'expert', None, None)

    def moe_body(x_act, route_idx, route_wts, w_one, w_three, w_two, dy_act):
        n_tok, model_dim = x_act.shape[1:]
        n_local = w_one.shape[1]
        n_rows = n_tok * n_dev
        n_col = model_dim // LANES
        w_in_one, w_in_three, w_out = w_one[0], w_three[0], w_two[0]

        def gather_tokens(rows):
            return lax.all_gather(rows, 'expert', axis=0, tiled=True)

        def scatter_sums(partial):
            own = lax.psum_scatter(partial, 'expert', scatter_dimension=0, tiled=True)
            return own.reshape(-1, model_dim).astype(BF16)

        n_list = n_local * LIST

        def to_experts(lists, dummy):
            lists = lax.all_to_all(lists.reshape(n_dev, n_list), 'expert', 0, 0, tiled=True)
            return jnp.concatenate([lists.reshape(n_dev * n_list), jnp.full((LANES,), dummy, lists.dtype)])

        idx_dst = lax.ppermute(route_idx[0], 'stage', to_next)
        wts_dst = lax.ppermute(route_wts[0], 'stage', to_next)
        idx_dst, wts_dst, x_src = lax.optimization_barrier((idx_dst, wts_dst, x_act[0]))
        x_dst = lax.ppermute(x_src, 'stage', to_next)
        dy_all = gather_tokens(dy_act[0])
        idx_dst = idx_dst.reshape(-1)
        wts_dst = wts_dst.reshape(-1)
        first_row = (lax.axis_index('expert') * n_tok).reshape(1)
        tok = route_lists(idx_dst, first_row, n_tok, n_local, n_dev, n_rows * n_col)
        x_dst, tok, idx_dst, wts_dst, x_again = lax.optimization_barrier((x_dst, tok, idx_dst, wts_dst, x_act[0]))
        x_all = gather_tokens(x_dst)
        x_dst_again = lax.ppermute(x_again, 'stage', to_next)
        g = route_lists(idx_dst, wts_dst, n_tok, n_local, n_dev, 0.0)
        tok, g = to_experts(tok, n_rows * n_col), to_experts(g, 0.0)
        tok, g, x_dst_again, dy_all, x_all = lax.optimization_barrier((tok, g, x_dst_again, dy_all, x_all))
        x_all_again = gather_tokens(x_dst_again)

        y_sum, d_rows, tiles = forward_partial(tok, g, x_all, dy_all, w_in_one, w_in_three, w_out, n_dev)
        y_sum, x_all_again, d_rows = lax.optimization_barrier((y_sum, x_all_again, d_rows))
        y_dst = scatter_sums(y_sum)

        (dx_low, dx_high), (x_rows, hidden, d_one, d_three) = backward_partial(tok, x_all_again, d_rows, w_in_one, w_in_three, w_out, n_dev, (0, n_tok * 3 // 4, n_tok))
        dx_low = scatter_sums(dx_low)
        dx_high = scatter_sums(dx_high)
        dx_low = lax.ppermute(dx_low, 'stage', to_prev)
        dx_high = lax.ppermute(dx_high, 'stage', to_prev)
        early = n_local * 7 // 8
        grads = weight_grads(tiles, x_rows, d_rows, hidden, d_one, d_three, n_dev, 0, early, ())
        g_one, g_three, g_two = weight_grads(tiles, x_rows, d_rows, hidden, d_one, d_three, n_dev, early, n_local - early, grads)
        dx_src = jnp.concatenate([dx_low, dx_high])
        return y_dst[None], dx_src[None], g_one[None], g_three[None], g_two[None]

    return jax.shard_map(moe_body, mesh=mesh, in_specs=(tok_spec, tok_spec, tok_spec, w_spec, w_spec, w_spec, tok_spec), out_specs=(tok_spec, tok_spec, w_spec, w_spec, w_spec), check_vma=False)
```

```python
import functools

import jax
import jax.numpy as jnp
from jax import lax
from jax.experimental import pallas as pl
from jax.experimental.pallas import tpu as pltpu
from jax.sharding import PartitionSpec as P


F32 = jnp.float32
BF16 = jnp.bfloat16
LIST = 264
GROUP = 8
PER_SRC = 256
TILE = 256
TILE_GROUPS = TILE // GROUP
LANES = 128
SUB = 4
FFN_STEP = 256
STAGE_ROWS = 128
STAGE_SLOTS = 8
VMEM_LIMIT = 66 * 1000 * 1000


def dot_nn(a, b):
    return lax.dot_general(a, b, (((1,), (0,)), ((), ())), preferred_element_type=F32)


def dot_nt(a, b):
    return lax.dot_general(a, b, (((1,), (1,)), ((), ())), preferred_element_type=F32)


def dot_tn(a, b):
    return lax.dot_general(a, b, (((0,), (0,)), ((), ())), preferred_element_type=F32)


def route_kernel(n_tok, top_k, n_local, n_dev, dummy, idx_ref, val_ref, out_ref, ptr_ref):
    per_pair = val_ref.shape[0] > 1

    @pl.loop(0, n_local * n_dev)
    def _(e):
        ptr_ref[e] = e * LIST

    @pl.loop(0, n_tok)
    def _(t):
        token = None if per_pair else (val_ref[0] + t) * SUB
        half = top_k // 2
        for part in range(2):
            at = t * top_k + part * half
            experts = [idx_ref[at + j] for j in range(half)]
            ptrs = [ptr_ref[e] for e in experts]
            vals = [val_ref[at + j] if per_pair else token for j in range(half)]
            for e, p, v in zip(experts, ptrs, vals):
                out_ref[p] = v
                ptr_ref[e] = p + 1

    @pl.loop(0, n_local * n_dev)
    def _(e):
        p = ptr_ref[e]
        for k in range(GROUP - 1):
            out_ref[p + k] = dummy
        out_ref[e * LIST + LIST - 1] = (p - e * LIST).astype(out_ref.dtype)


def route_lists(idx, vals, n_tok, n_local, n_dev, dummy):
    n_pair = idx.shape[0]
    smem = pl.BlockSpec(memory_space=pltpu.SMEM)
    return pl.pallas_call(
        functools.partial(route_kernel, n_tok, n_pair // n_tok, n_local, n_dev, dummy),
        out_shape=jax.ShapeDtypeStruct((n_dev * n_local * LIST,), vals.dtype),
        in_specs=[smem, smem],
        out_specs=smem,
        scratch_shapes=[pltpu.SMEM((n_local * n_dev,), jnp.int32)],
        cost_estimate=pl.CostEstimate(flops=40 * 10**8, bytes_accessed=8 * n_local * n_dev * LIST, transcendentals=0),
        name='route_lists',
    )(idx, vals)


def load_table(src_hbm, table, stage, sem, n_rows, n_col):
    n_chunk = n_rows // STAGE_ROWS

    def fetch(i):
        slot = lax.rem(i, STAGE_SLOTS)
        return pltpu.make_async_copy(src_hbm.at[pl.ds(pl.multiple_of(i * STAGE_ROWS, STAGE_ROWS), STAGE_ROWS)], stage.at[slot], sem.at[slot])

    for k in range(min(STAGE_SLOTS, n_chunk)):
        fetch(jnp.int32(k)).start()

    @pl.loop(0, n_chunk)
    def _(i):
        fetch(i).wait()
        rows = stage[lax.rem(i, STAGE_SLOTS)]
        for c in range(n_col):
            table[pl.ds(i * (STAGE_ROWS * n_col) + c, STAGE_ROWS, stride=n_col), :] = rows[:, c * LANES:(c + 1) * LANES].astype(F32)

        @pl.when(i + STAGE_SLOTS < n_chunk)
        def _():
            fetch(i + STAGE_SLOTS).start()

    table[pl.ds(n_rows * n_col, 8), :] = jnp.zeros((8, LANES), F32)


SLOT = 4 * (PER_SRC // GROUP) + TILE_GROUPS + 16


def rows_at(first, n_col):
    return pl.ds(pl.multiple_of(first, n_col), n_col)


def n_groups(tok, p, e, n_local):
    return lax.div(tok[(p * n_local + e) * LIST + LIST - 1] + (GROUP - 1), GROUP)


def all_groups(tok, e, n_src, n_local):
    groups = n_groups(tok, 0, e, n_local)
    for p in range(1, n_src):
        groups = groups + n_groups(tok, p, e, n_local)
    return groups


def n_tiles(tok, e, n_src, n_local):
    return lax.div(all_groups(tok, e, n_src, n_local) + (TILE_GROUPS - 1), TILE_GROUPS)


def list_groups(tok, grp, e, n_src, n_local):
    empty = n_src * n_local * LIST
    at = lax.rem(e, 3) * SLOT
    for p in range(n_src):
        base = (p * n_local + e) * LIST
        groups = n_groups(tok, p, e, n_local)

        @pl.loop(0, lax.div(groups + 3, 4))
        def _(i, base=base, at=at):
            for k in range(4):
                grp[at + 4 * i + k] = base + (4 * i + k) * GROUP

        at = at + groups
    for k in range(TILE_GROUPS):
        grp[at + k] = empty


def start_groups(tok, grp, n_src, n_local):
    for k in range(TILE_GROUPS):
        grp[3 * SLOT + k] = n_src * n_local * LIST
    list_groups(tok, grp, jnp.int32(0), n_src, n_local)


def pick_group(tok, g, tables, bufs, base, row, n_col):
    for k in range(GROUP):
        src = rows_at(tok[base + k], n_col)
        dst = pl.ds(row * n_col + k * n_col, n_col)
        bufs[0][dst, :] = tables[0][src, :]
        if len(tables) > 1:
            bufs[1][dst, :] = tables[1][src, :] * g[base + k]


def add_group(tok, g, acc, buf, base, row, n_col, step):
    for first in range(0, GROUP, step):
        dsts, rows = [], []
        for k in range(first, first + step):
            dsts.append(rows_at(tok[base + k], n_col))
            val = buf[pl.ds((row + k) * n_col, n_col), :]
            rows.append(val if g is None else val * g[base + k])
        sums = [acc[d, :] + r for d, r in zip(dsts, rows)]
        for d, r in zip(dsts, sums):
            acc[d, :] = r


def tile_rows(buf, n_col, n_rows=TILE):
    return jnp.concatenate([buf[pl.ds(c, n_rows, stride=n_col), :] for c in range(n_col)], axis=1).astype(BF16)


def put_rows(buf, rows, n_col):
    for c in range(n_col):
        buf[pl.ds(c, rows.shape[0], stride=n_col), :] = rows[:, c * LANES:(c + 1) * LANES].astype(F32)


def pipelined_tiles(e, n_src, n_local, n_col, tok, g, grp, prev, tables, pick_bufs, acc, out_buf, step, halves, compute):
    groups = all_groups(tok, e, n_src, n_local)
    tiles = n_tiles(tok, e, n_src, n_local)
    here = lax.rem(e, 3) * SLOT
    following = lax.rem(e + 1, 3) * SLOT

    @pl.when(e == 0)
    def _():
        prev[0] = 3 * SLOT
        start_groups(tok, grp, n_src, n_local)

        @pl.loop(0, TILE_GROUPS)
        def _(q):
            pick_group(tok, g, tables, pick_bufs, grp[q], pl.multiple_of(q * GROUP, GROUP), n_col)

    list_groups(tok, grp, lax.min(e + 1, n_local - 1), n_src, n_local)

    @pl.loop(0, tiles)
    def _(i):
        last = prev[0]
        coming = jnp.where(i + 1 < tiles, here + (i + 1) * TILE_GROUPS, following)

        def side(part, parts):
            for q in range(part * TILE_GROUPS // parts, (part + 1) * TILE_GROUPS // parts):
                add_group(tok, g, acc, out_buf, grp[last + q], q * GROUP, n_col, step)
                pick_group(tok, g, tables, pick_bufs, grp[coming + q], q * GROUP, n_col)

        if halves:
            short = groups - i * TILE_GROUPS <= TILE_GROUPS // 2

            @pl.when(short)
            def _():
                compute(i, TILE // 2, side)

            @pl.when(jnp.logical_not(short))
            def _():
                compute(i, TILE, side)
        else:
            compute(i, TILE, side)

        prev[0] = here + i * TILE_GROUPS

    @pl.when(e == n_local - 1)
    def _():
        @pl.loop(0, TILE_GROUPS)
        def _(q):
            add_group(tok, g, acc, out_buf, grp[prev[0] + q], pl.multiple_of(q * GROUP, GROUP), n_col, step)


def forward_kernel(n_src, n_local, n_rows, n_col, tok_hbm, g_hbm, x_hbm, dy_hbm, w_one, w_three, w_two, y_hbm, d_ref, tiles_ref, x_table, d_table, acc, x_buf, d_buf, out_buf, stage, grp, prev, sem, list_sem, tok, g):
    e = pl.program_id(0)

    @pl.when(e == 0)
    def _():
        lists = [pltpu.make_async_copy(tok_hbm, tok, list_sem.at[0]), pltpu.make_async_copy(g_hbm, g, list_sem.at[1])]
        for copy in lists:
            copy.start()
        acc[...] = jnp.zeros_like(acc)
        load_table(x_hbm, x_table, stage, sem, n_rows, n_col)
        load_table(dy_hbm, d_table, stage, sem, n_rows, n_col)
        for copy in lists:
            copy.wait()

    tiles_ref[e] = n_tiles(tok, e, n_src, n_local)

    def compute(i, used, side):
        rows = pl.ds(pl.multiple_of(i * TILE, TILE), TILE)
        x = tile_rows(x_buf, n_col, used)
        d_ref[0, rows, :] = tile_rows(d_buf, n_col)
        ffn = w_one.shape[2]
        hidden = []
        for k, f in enumerate(range(0, ffn, FFN_STEP)):
            side(k, ffn // FFN_STEP)
            pre_one = dot_nn(x, w_one[0, :, f:f + FFN_STEP])
            pre_three = dot_nn(x, w_three[0, :, f:f + FFN_STEP])
            hidden.append((pre_one * jax.nn.sigmoid(pre_one) * pre_three).astype(BF16))
        put_rows(out_buf, dot_nn(jnp.concatenate(hidden, axis=1), w_two[0]).astype(BF16), n_col)

    pipelined_tiles(e, n_src, n_local, n_col, tok, g, grp, prev, (x_table, d_table), (x_buf, d_buf), acc, out_buf, GROUP, False, compute)

    @pl.when(e == n_local - 1)
    def _():
        out = pltpu.make_async_copy(acc.at[pl.ds(0, n_rows * n_col)], y_hbm, sem.at[0])
        out.start()
        out.wait()


def kernel_scratch(n_rows, model, n_table, n_pick):
    n_col = model // LANES
    table = pltpu.VMEM((n_rows * n_col + 8, LANES), F32)
    tile = pltpu.VMEM((TILE * n_col, LANES), F32)
    return [table] * (n_table + 1) + [tile] * (n_pick + 1) + [
        pltpu.VMEM((STAGE_SLOTS, STAGE_ROWS, model), BF16),
        pltpu.SMEM((3 * SLOT + TILE_GROUPS,), jnp.int32),
        pltpu.SMEM((1,), jnp.int32),
        pltpu.SemaphoreType.DMA((STAGE_SLOTS,)),
        pltpu.SemaphoreType.DMA((2,)),
    ]


def per_expert(a, b):
    return pl.BlockSpec((1, a, b), lambda e: (e, 0, 0))


def forward_partial(tok, g, x_all, dy_all, w_one, w_three, w_two, n_src):
    n_rows, model = x_all.shape
    n_local, _, ffn = w_one.shape
    n_col = model // LANES
    cap = n_src * PER_SRC
    smem = pl.BlockSpec(memory_space=pltpu.SMEM)
    hbm = pl.BlockSpec(memory_space=pl.ANY)
    pairs = n_rows * 8 // n_src
    return pl.pallas_call(
        functools.partial(forward_kernel, n_src, n_local, n_rows, n_col),
        out_shape=(jax.ShapeDtypeStruct((n_rows * n_col, LANES), F32), jax.ShapeDtypeStruct((n_local, cap, model), BF16), jax.ShapeDtypeStruct((n_local,), jnp.int32)),
        grid=(n_local,),
        in_specs=[hbm, hbm, hbm, hbm, per_expert(model, ffn), per_expert(model, ffn), per_expert(ffn, model)],
        out_specs=(hbm, per_expert(cap, model), smem),
        scratch_shapes=kernel_scratch(n_rows, model, 2, 2) + [pltpu.SMEM(tok.shape, tok.dtype), pltpu.SMEM(g.shape, g.dtype)],
        compiler_params=pltpu.CompilerParams(dimension_semantics=('arbitrary',), vmem_limit_bytes=VMEM_LIMIT),
        cost_estimate=pl.CostEstimate(flops=6 * pairs * model * ffn, bytes_accessed=6 * n_local * model * ffn, transcendentals=0),
        name='forward_partial',
    )(tok, g, x_all, dy_all, w_one, w_three, w_two)


def backward_kernel(n_src, n_local, n_rows, n_col, cuts, tok_hbm, x_hbm, d_ref, w_one, w_three, w_two, *rest):
    n_part = len(cuts) - 1
    parts, rest = rest[:n_part], rest[n_part:]
    x_ref, h_ref, d1_ref, d3_ref, table, acc, x_buf, out_buf, stage, grp, prev, sem, list_sem, tok = rest
    e = pl.program_id(0)

    @pl.when(e == 0)
    def _():
        lists = pltpu.make_async_copy(tok_hbm, tok, list_sem.at[0])
        lists.start()
        acc[...] = jnp.zeros_like(acc)
        load_table(x_hbm, table, stage, sem, n_rows, n_col)
        lists.wait()

    def compute(i, used, side):
        rows = pl.ds(pl.multiple_of(i * TILE, TILE), TILE)
        x = tile_rows(x_buf, n_col)
        x_ref[0, rows, :] = x
        x = x[:used]
        if used < TILE:
            unused = pl.ds(pl.multiple_of(i * TILE + used, TILE // 2), TILE - used)
            for ref in (h_ref, d1_ref, d3_ref):
                ref[0, unused, :] = jnp.zeros((TILE - used, ref.shape[2]), BF16)
        rows = pl.ds(pl.multiple_of(i * TILE, TILE), used)
        d = d_ref[0, rows, :]
        ffn = w_one.shape[2]
        for k, f in enumerate(range(0, ffn, FFN_STEP)):
            cols = slice(f, f + FFN_STEP)
            side(k, ffn // FFN_STEP)
            pre_one = dot_nn(x, w_one[0, :, cols])
            pre_three = dot_nn(x, w_three[0, :, cols])
            d_hidden = dot_nt(d, w_two[0, cols, :]).astype(BF16).astype(F32)
            sig_one = jax.nn.sigmoid(pre_one)
            act_one = pre_one * sig_one
            h_ref[0, rows, cols] = (act_one * pre_three).astype(BF16)
            d3_ref[0, rows, cols] = (d_hidden * act_one).astype(BF16)
            d1_ref[0, rows, cols] = (d_hidden * pre_three * sig_one * (1.0 + pre_one * (1.0 - sig_one))).astype(BF16)
        dx = dot_nt(d1_ref[0, rows, :], w_one[0]) + dot_nt(d3_ref[0, rows, :], w_three[0])
        put_rows(out_buf, dx.astype(BF16), n_col)

    pipelined_tiles(e, n_src, n_local, n_col, tok, None, grp, prev, (table,), (x_buf,), acc, out_buf, GROUP // 2, True, compute)

    @pl.when(e == n_local - 1)
    def _():
        own = n_rows * n_col // n_src
        outs = []
        for k, (lo, hi) in enumerate(zip(cuts, cuts[1:])):
            part = (hi - lo) * n_col
            outs += [pltpu.make_async_copy(acc.at[pl.ds(q * own + lo * n_col, part)], parts[k].at[pl.ds(q * part, part)], sem.at[0]) for q in range(n_src)]
        for out in outs:
            out.start()
        for out in outs:
            out.wait()


def backward_partial(tok, x_all, d_rows, w_one, w_three, w_two, n_src, cuts):
    n_rows, model = x_all.shape
    n_local, cap, _ = d_rows.shape
    ffn = w_one.shape[2]
    n_col = model // LANES
    hbm = pl.BlockSpec(memory_space=pl.ANY)
    ffn_out = jax.ShapeDtypeStruct((n_local, cap, ffn), BF16)
    pairs = n_rows * 8 // n_src
    n_part = len(cuts) - 1
    outs = pl.pallas_call(
        functools.partial(backward_kernel, n_src, n_local, n_rows, n_col, cuts),
        out_shape=tuple(jax.ShapeDtypeStruct((n_src * (hi - lo) * n_col, LANES), F32) for lo, hi in zip(cuts, cuts[1:])) + (jax.ShapeDtypeStruct((n_local, cap, model), BF16), ffn_out, ffn_out, ffn_out),
        grid=(n_local,),
        in_specs=[hbm, hbm, per_expert(cap, model), per_expert(model, ffn), per_expert(model, ffn), per_expert(ffn, model)],
        out_specs=(hbm,) * n_part + (per_expert(cap, model), per_expert(cap, ffn), per_expert(cap, ffn), per_expert(cap, ffn)),
        scratch_shapes=kernel_scratch(n_rows, model, 1, 1) + [pltpu.SMEM(tok.shape, tok.dtype)],
        compiler_params=pltpu.CompilerParams(dimension_semantics=('arbitrary',), vmem_limit_bytes=VMEM_LIMIT),
        cost_estimate=pl.CostEstimate(flops=10 * pairs * model * ffn, bytes_accessed=6 * n_local * cap * ffn, transcendentals=0),
        name='backward_partial',
    )(tok, x_all, d_rows, w_one, w_three, w_two)
    return outs[:n_part], outs[n_part:]


def grad_kernel(n_src, first, tiles, x_ref, d_ref, h_ref, d1_ref, d3_ref, *refs):
    g1_ref, g3_ref, g2_ref = refs[-3:]
    used = tiles[pl.program_id(0) + first]
    for n in range(1, n_src * PER_SRC // TILE + 1):
        @pl.when(used == n)
        def _(n=n):
            rows = pl.ds(0, n * TILE)
            g1_ref[0] = dot_tn(x_ref[0, rows, :], d1_ref[0, rows, :]).astype(BF16)
            g3_ref[0] = dot_tn(x_ref[0, rows, :], d3_ref[0, rows, :]).astype(BF16)
            g2_ref[0] = dot_tn(h_ref[0, rows, :], d_ref[0, rows, :]).astype(BF16)


def weight_grads(tiles, x_rows, d_rows, hidden, d_one, d_three, n_src, first, count, so_far):
    n_local, cap, model = x_rows.shape
    ffn = hidden.shape[2]
    block = lambda a, b: pl.BlockSpec((1, a, b), lambda e: (e + first, 0, 0))
    in_grad = jax.ShapeDtypeStruct((n_local, model, ffn), BF16)
    pairs = count * cap // 2
    return pl.pallas_call(
        functools.partial(grad_kernel, n_src, first),
        out_shape=(in_grad, in_grad, jax.ShapeDtypeStruct((n_local, ffn, model), BF16)),
        grid=(count,),
        in_specs=[pl.BlockSpec(memory_space=pltpu.SMEM), block(cap, model), block(cap, model), block(cap, ffn), block(cap, ffn), block(cap, ffn)] + [pl.BlockSpec(memory_space=pl.ANY)] * len(so_far),
        out_specs=(block(model, ffn), block(model, ffn), block(ffn, model)),
        input_output_aliases={6 + k: k for k in range(len(so_far))},
        compiler_params=pltpu.CompilerParams(dimension_semantics=('arbitrary',), vmem_limit_bytes=VMEM_LIMIT),
        cost_estimate=pl.CostEstimate(flops=6 * pairs * model * ffn, bytes_accessed=6 * count * cap * ffn, transcendentals=0),
        name='weight_grads',
    )(tiles, x_rows, d_rows, hidden, d_one, d_three, *so_far)


def solution(mesh):
    n_stage = mesh.shape['stage']
    n_dev = mesh.shape['expert']
    to_next = [(stage_idx, (stage_idx + 1) % n_stage) for stage_idx in range(n_stage)]
    to_prev = [((stage_idx + 1) % n_stage, stage_idx) for stage_idx in range(n_stage)]
    tok_spec = P('stage', 'expert', None)
    w_spec = P('stage', 'expert', None, None)

    def moe_body(x_act, route_idx, route_wts, w_one, w_three, w_two, dy_act):
        n_tok, model_dim = x_act.shape[1:]
        n_local = w_one.shape[1]
        n_rows = n_tok * n_dev
        n_col = model_dim // LANES
        w_in_one, w_in_three, w_out = w_one[0], w_three[0], w_two[0]

        def gather_tokens(rows):
            return lax.all_gather(rows, 'expert', axis=0, tiled=True)

        def scatter_sums(partial):
            own = lax.psum_scatter(partial, 'expert', scatter_dimension=0, tiled=True)
            return own.reshape(-1, model_dim).astype(BF16)

        n_list = n_local * LIST

        def to_experts(lists, dummy):
            lists = lax.all_to_all(lists.reshape(n_dev, n_list), 'expert', 0, 0, tiled=True)
            return jnp.concatenate([lists.reshape(n_dev * n_list), jnp.full((LANES,), dummy, lists.dtype)])

        idx_dst = lax.ppermute(route_idx[0], 'stage', to_next)
        wts_dst = lax.ppermute(route_wts[0], 'stage', to_next)
        idx_dst, wts_dst, x_src = lax.optimization_barrier((idx_dst, wts_dst, x_act[0]))
        x_dst = lax.ppermute(x_src, 'stage', to_next)
        dy_all = gather_tokens(dy_act[0])
        idx_dst = idx_dst.reshape(-1)
        wts_dst = wts_dst.reshape(-1)
        first_row = (lax.axis_index('expert') * n_tok).reshape(1)
        tok = route_lists(idx_dst, first_row, n_tok, n_local, n_dev, n_rows * n_col)
        x_dst, tok, idx_dst, wts_dst, x_again = lax.optimization_barrier((x_dst, tok, idx_dst, wts_dst, x_act[0]))
        x_all = gather_tokens(x_dst)
        x_dst_again = lax.ppermute(x_again, 'stage', to_next)
        g = route_lists(idx_dst, wts_dst, n_tok, n_local, n_dev, 0.0)
        tok, g = to_experts(tok, n_rows * n_col), to_experts(g, 0.0)
        tok, g, x_dst_again, dy_all, x_all = lax.optimization_barrier((tok, g, x_dst_again, dy_all, x_all))
        x_all_again = gather_tokens(x_dst_again)

        y_sum, d_rows, tiles = forward_partial(tok, g, x_all, dy_all, w_in_one, w_in_three, w_out, n_dev)
        y_sum, x_all_again, d_rows = lax.optimization_barrier((y_sum, x_all_again, d_rows))
        y_dst = scatter_sums(y_sum)

        (dx_low, dx_high), (x_rows, hidden, d_one, d_three) = backward_partial(tok, x_all_again, d_rows, w_in_one, w_in_three, w_out, n_dev, (0, n_tok * 3 // 4, n_tok))
        dx_low = scatter_sums(dx_low)
        dx_high = scatter_sums(dx_high)
        dx_low = lax.ppermute(dx_low, 'stage', to_prev)
        dx_high = lax.ppermute(dx_high, 'stage', to_prev)
        early = n_local * 7 // 8
        grads = weight_grads(tiles, x_rows, d_rows, hidden, d_one, d_three, n_dev, 0, early, ())
        g_one, g_three, g_two = weight_grads(tiles, x_rows, d_rows, hidden, d_one, d_three, n_dev, early, n_local - early, grads)
        dx_src = jnp.concatenate([dx_low, dx_high])
        return y_dst[None], dx_src[None], g_one[None], g_three[None], g_two[None]

    return jax.shard_map(moe_body, mesh=mesh, in_specs=(tok_spec, tok_spec, tok_spec, w_spec, w_spec, w_spec, tok_spec), out_specs=(tok_spec, tok_spec, w_spec, w_spec, w_spec), check_vma=False)
```
